32 devices in a mesh: runs: 2 (over y), lon: 4 (over x, core), lat: 4 (over z).
Axes of the slice: x: 2, y: 2, z: 4, core: 2. Of those that a mesh axis runs over, the one named last changes fastest.
Arguments:
- latent: bfloat16 [8, 24, 48, 512], P('runs', 'lat', 'lon'), parts along dimension 0, may hold values from -16 to 16
- cotangent: bfloat16 [8, 24, 48, 512], P('runs', 'lat', 'lon'), parts along dimension 0, may hold values from -6 to 6
- mask_ids: int32 [8, 24, 48], P('runs', 'lat', 'lon'), parts along dimension 0, may hold values from 0 to 1
- position_bias: float32 [8, 37], replicated, may hold values from -2 to 302
- norm_gain: float32 [512], replicated, may hold values from 0.1 to 1.9
- w_qkv: bfloat16 [512, 1536], replicated, may hold values from -0.25 to 0.25
- qkv_down: bfloat16 [16, 512], replicated, may hold values from -0.25 to 0.25
- qkv_up: bfloat16 [16, 1536], replicated, may hold values from -0.75 to 0.75
- w_proj: bfloat16 [512, 512], replicated, may hold values from -0.25 to 0.25
- proj_down: bfloat16 [16, 512], replicated, may hold values from -0.25 to 0.25
- proj_up: bfloat16 [16, 512], replicated, may hold values from -0.75 to 0.75
Outputs:
- output: bfloat16 [8, 24, 48, 512], P('runs', 'lat', 'lon'), parts along dimension 0
- latent_grad: bfloat16 [8, 24, 48, 512], P('runs', 'lat', 'lon'), parts along dimension 0
- qkv_down_grad: float32 [32, 512], P('runs'), parts along dimension 0
- qkv_up_grad: float32 [32, 1536], P('runs'), parts along dimension 0
- proj_down_grad: float32 [32, 512], P('runs'), parts along dimension 0
- proj_up_grad: float32 [32, 512], P('runs'), parts along dimension 0
The draws below stay inside these ranges and needn't reach their ends.
There are 2 independent parts, one for each index of `runs`. The reference program is written for one: setup_inputs(seed, part) draws one part's arguments, and reference() takes and returns one part's arrays. A program takes and returns all parts, laid end to end along the dimension named above; an argument that names none is the same for every part. Nothing has to cross between parts.
All inputs are finite; a program needn't handle non-finite values.
Results may differ from the reference program's by a relative error of at most 0.011.
Values may be sent and summed in bfloat16 or wider, within the bound.
No kernel may reach another device: no remote copies, remote signals or barrier semaphores. Data moves between devices by JAX's collectives and lax.ppermute only.
A program may use at most 64 MiB of HBM per device.

```python
import math
import jax
import jax.numpy as jnp
from jax import lax

D = 512
HEADS = 8
LEVELS = 4
RANK = 16
WIN_LEV = 2
WIN_LAT = 6
WIN_LON = 12
LAT = 24
LON = 48
TOKENS = 4608
BIAS_COLS = 37


def draw_latent(key, part):
    key_base = jax.random.fold_in(key, 0)
    shape = (LEVELS, LAT, LON, D)
    values = jax.random.normal(key_base, shape, jnp.float32)
    return jnp.clip(values, -16.0, 16.0).astype(jnp.bfloat16)


def draw_position_bias(key, part):
    key_base = jax.random.fold_in(jax.random.fold_in(key, 17), 0)
    base = jax.random.uniform(key_base, (HEADS, BIAS_COLS), jnp.float32, -2.0, 2.0)
    values = base
    return values


def plant(result, key, least, largest):
    index_at = [jax.random.randint(jax.random.fold_in(key, axis), (), 0, length) for axis, length in enumerate(result.shape)]
    widest = result.shape.index(max(result.shape))
    neighbour = index_at[:widest] + [(index_at[widest] + 1) % result.shape[widest]] + index_at[widest + 1:]
    return result.at[tuple(index_at)].set(least).at[tuple(neighbour)].set(largest)


def level_of(rng, dims, cuts, smallest, top_value):
    def one(axis_at, shards_of):
        heights = jax.random.uniform(jax.random.fold_in(jax.random.fold_in(rng, 6), axis_at), (shards_of,), jnp.float32, smallest / len(cuts), top_value / len(cuts))
        return jnp.repeat(jnp.exp(heights), dims[axis_at] // shards_of).reshape((-1,) + (1,) * (len(dims) - axis_at - 1))

    gain = one(*cuts[0])
    for cut in cuts[1:]:
        gain = gain * one(*cut)
    return gain


def noise(stream_key, extent, deviation, most, shards=(), kind=jnp.bfloat16):
    values = deviation * jax.random.normal(stream_key, extent, jnp.float32)
    if shards:
        values = values * level_of(stream_key, extent, shards, -0.22, 0.18)
    return jnp.clip(values, -most, most).astype(kind)


def setup_inputs(seed: int = 0, part: int = 0) -> dict:
    splits = jax.random.split(jax.random.key(seed), 12)
    own_keys = jax.random.split(jax.random.fold_in(splits[11], part), 12)
    return {
        "latent": draw_latent(jax.random.fold_in(jax.random.fold_in(splits[11], part), 71), part),
        "cotangent": noise(own_keys[1], (LEVELS, LAT, LON, D), 1.0, 6.0, ((1, 4), (2, 4))),
        "mask_ids": plant(jax.random.randint(own_keys[2], (LEVELS, LAT, LON), 0, 2), jax.random.fold_in(own_keys[2], 1), 0, 1).astype(jnp.int32),
        "position_bias": draw_position_bias(jax.random.fold_in(splits[11], 71), part),
        "norm_gain": jnp.clip(1.0 + 0.18 * jax.random.normal(splits[4], (D,), jnp.float32), 0.1, 1.9),
        "w_qkv": noise(splits[5], (D, 3 * D), D ** -0.5, 0.25),
        "qkv_down": noise(splits[6], (RANK, D), D ** -0.5, 0.25),
        "qkv_up": noise(splits[7], (RANK, 3 * D), (4 * RANK) ** -0.5, 0.75),
        "w_proj": noise(splits[8], (D, D), D ** -0.5, 0.25),
        "proj_down": noise(splits[9], (RANK, D), D ** -0.5, 0.25),
        "proj_up": noise(splits[10], (RANK, D), (4 * RANK) ** -0.5, 0.75),
    }


epsilon = 1e-05
masked_value = -1e+30

def widen(array_in):
    return array_in.astype(jnp.float32)

def dot_rows(left_side, right_side):
    return lax.dot_general(widen(left_side), widen(right_side), (((1,), (1,)), ((), ())))

def dot_cols(left_side, right_side):
    return lax.dot_general(widen(left_side), widen(right_side), (((0,), (0,)), ((), ())))

def window_bias(position_bias):
    window_size = WIN_LEV * WIN_LAT * WIN_LON
    places = jnp.arange(window_size, dtype=jnp.int32)
    level_pos = places // (WIN_LAT * WIN_LON)
    lat_pos = places // WIN_LON % WIN_LAT
    lon_pos = places % WIN_LON
    level_col = level_pos[:, None] - level_pos[None, :] + WIN_LEV - 1
    lat_col = lat_pos[:, None] - lat_pos[None, :] + 2 * WIN_LEV - 1 + WIN_LAT - 1
    lon_col = lon_pos[:, None] - lon_pos[None, :] + 2 * WIN_LEV + 2 * WIN_LAT - 2 + WIN_LON - 1
    columns = jnp.arange(position_bias.shape[1], dtype=jnp.int32)[:, None, None]
    one_hot = (columns == level_col[None]) | (columns == lat_col[None]) | (columns == lon_col[None])
    one_hot = one_hot.astype(jnp.float32).reshape(position_bias.shape[1], window_size * window_size)
    table = jnp.dot(position_bias, one_hot, precision=lax.Precision.HIGHEST)
    return table.reshape(position_bias.shape[0], window_size, window_size)

def to_windows(grid):
    levels, lat_rows, lon_cols, chans = grid.shape
    blocks = grid.reshape(levels // WIN_LEV, WIN_LEV, lat_rows // WIN_LAT, WIN_LAT, lon_cols // WIN_LON, WIN_LON, chans)
    return blocks.transpose(0, 2, 4, 1, 3, 5, 6).reshape(-1, WIN_LEV * WIN_LAT * WIN_LON, chans)

def from_windows(windows, levels, lat_rows, lon_cols):
    chans = windows.shape[-1]
    blocks = windows.reshape(levels // WIN_LEV, lat_rows // WIN_LAT, lon_cols // WIN_LON, WIN_LEV, WIN_LAT, WIN_LON, chans)
    return blocks.transpose(0, 3, 1, 4, 2, 5, 6).reshape(levels, lat_rows, lon_cols, chans)

def window_pass(x_block, g_block, id_block, bias_table, norm_gain, w_qkv, qkv_down, qkv_up, w_proj, proj_down, proj_up):
    windows, window_size, width = x_block.shape
    rows_total = windows * window_size
    head_size = width // HEADS
    score_scale = 1.0 / math.sqrt(head_size)
    flat_rows = widen(x_block.reshape(rows_total, width))
    average = lax.optimization_barrier(jnp.mean(flat_rows, axis=-1, keepdims=True))
    centered = flat_rows - average
    variance = lax.optimization_barrier(jnp.mean(centered * centered, axis=-1, keepdims=True))
    inv_std = lax.rsqrt(variance + epsilon)
    unit_rows = centered * inv_std
    normed = (unit_rows * norm_gain).astype(jnp.bfloat16)
    low_qkv = dot_rows(normed, qkv_down).astype(jnp.bfloat16)
    qkv = (jnp.dot(widen(normed), w_qkv) + jnp.dot(widen(low_qkv), widen(qkv_up))).astype(jnp.bfloat16)
    pieces = qkv.reshape(windows, window_size, 3, HEADS, head_size)
    query, keys, values = (pieces[:, :, 0], pieces[:, :, 1], pieces[:, :, 2])
    allowed = id_block[:, None, :, None] == id_block[:, None, None, :]
    scores = jnp.einsum('bqhd,bkhd->bhqk', widen(query), widen(keys)) * score_scale + bias_table[None]
    scores = jnp.where(allowed, scores, masked_value)
    row_max = lax.optimization_barrier(jnp.max(scores, axis=-1, keepdims=True))
    exp_terms = jnp.where(allowed, jnp.exp(scores - row_max), 0.0)
    probs_full = exp_terms / lax.optimization_barrier(jnp.sum(exp_terms, axis=-1, keepdims=True))
    probs = probs_full.astype(jnp.bfloat16)
    attn = jnp.einsum('bhqk,bkhd->bqhd', widen(probs), widen(values)).astype(jnp.bfloat16).reshape(rows_total, width)
    low_proj = dot_rows(attn, proj_down).astype(jnp.bfloat16)
    out_rows = (flat_rows + jnp.dot(widen(attn), widen(w_proj)) + jnp.dot(widen(low_proj), widen(proj_up))).astype(jnp.bfloat16)
    grad_rows = g_block.reshape(rows_total, width)
    proj_up_raw = dot_cols(low_proj, grad_rows)
    d_low_proj = dot_rows(grad_rows, proj_up).astype(jnp.bfloat16)
    proj_down_raw = dot_cols(d_low_proj, attn)
    d_attn = (dot_rows(grad_rows, w_proj) + jnp.dot(widen(d_low_proj), widen(proj_down))).astype(jnp.bfloat16)
    d_heads = d_attn.reshape(windows, window_size, HEADS, head_size)
    d_probs = jnp.einsum('bqhd,bkhd->bhqk', widen(d_heads), widen(values))
    d_values = jnp.einsum('bhqk,bqhd->bkhd', widen(probs), widen(d_heads))
    d_scores = (probs_full * (d_probs - lax.optimization_barrier(jnp.sum(d_probs * probs_full, axis=-1, keepdims=True))) * score_scale).astype(jnp.bfloat16)
    d_query = jnp.einsum('bhqk,bkhd->bqhd', widen(d_scores), widen(keys))
    d_keys = jnp.einsum('bhqk,bqhd->bkhd', widen(d_scores), widen(query))
    d_qkv = jnp.stack([d_query, d_keys, d_values], axis=2).astype(jnp.bfloat16).reshape(rows_total, 3 * width)
    qkv_up_raw = dot_cols(low_qkv, d_qkv)
    d_low_qkv = dot_rows(d_qkv, qkv_up).astype(jnp.bfloat16)
    qkv_down_raw = dot_cols(d_low_qkv, normed)
    d_normed = dot_rows(d_qkv, w_qkv) + jnp.dot(widen(d_low_qkv), widen(qkv_down))
    d_unit = d_normed * norm_gain
    norm_back = inv_std * (d_unit - lax.optimization_barrier(jnp.mean(d_unit, axis=-1, keepdims=True)) - unit_rows * lax.optimization_barrier(jnp.mean(d_unit * unit_rows, axis=-1, keepdims=True)))
    grad_in = (widen(grad_rows) + norm_back).astype(jnp.bfloat16)
    return (out_rows.reshape(x_block.shape), grad_in.reshape(x_block.shape), (qkv_down_raw, qkv_up_raw, proj_down_raw, proj_up_raw))

def reference(latent, cotangent, mask_ids, position_bias, norm_gain, w_qkv, qkv_down, qkv_up, w_proj, proj_down, proj_up):
    offsets = (-(WIN_LEV // 2), -(WIN_LAT // 2), -(WIN_LON // 2))
    backs = (WIN_LEV // 2, WIN_LAT // 2, WIN_LON // 2)
    shifted = jnp.roll(latent, offsets, axis=(0, 1, 2))
    grad_shifted = jnp.roll(cotangent, offsets, axis=(0, 1, 2))
    bias_table = window_bias(position_bias)
    wide_qkv = widen(w_qkv)
    window_size = WIN_LEV * WIN_LAT * WIN_LON
    x_windows = to_windows(shifted).reshape(-1, 8, window_size, D)
    g_windows = to_windows(grad_shifted).reshape(-1, 8, window_size, D)
    id_windows = to_windows(mask_ids[..., None])[..., 0].reshape(-1, 8, window_size)

    def block_step(totals, block):
        x_block, g_block, id_block = block
        out_block, grad_block, terms = window_pass(x_block, g_block, id_block, bias_table, norm_gain, wide_qkv, qkv_down, qkv_up, w_proj, proj_down, proj_up)
        return (tuple((total + term for total, term in zip(totals, terms))), (out_block, grad_block))
    initial = (jnp.zeros((RANK, D), jnp.float32), jnp.zeros((RANK, 3 * D), jnp.float32), jnp.zeros((RANK, D), jnp.float32), jnp.zeros((RANK, D), jnp.float32))
    totals, (out_blocks, grad_blocks) = lax.scan(block_step, initial, (x_windows, g_windows, id_windows))
    shifted_out = from_windows(out_blocks.reshape(-1, window_size, D), LEVELS, LAT, LON)
    grad_in = from_windows(grad_blocks.reshape(-1, window_size, D), LEVELS, LAT, LON)
    output = jnp.roll(shifted_out, backs, axis=(0, 1, 2))
    latent_grad = jnp.roll(grad_in, backs, axis=(0, 1, 2))
    grad_scale = 1.0 / math.sqrt(TOKENS)
    return (output, latent_grad, totals[0] * grad_scale, totals[1] * grad_scale, totals[2] * grad_scale, totals[3] * grad_scale)
```

```python
import math

import jax
import jax.numpy as jnp
import numpy as np
from jax import lax
from jax.experimental import pallas as pl
from jax.experimental.pallas import tpu as pltpu
from jax.sharding import PartitionSpec as P

HEADS = 8
WIN_LEV = 2
WIN_LAT = 6
WIN_LON = 12
HALF_LAT = WIN_LAT // 2
HALF_LON = WIN_LON // 2
HALF_LEV = WIN_LEV // 2
WINDOW = WIN_LEV * WIN_LAT * WIN_LON
QUAD = WINDOW // 4

epsilon = 1e-05
masked_value = -1e30
f32 = jnp.float32
bf16 = jnp.bfloat16


def nn(a, b):
    return lax.dot_general(a, b, (((1,), (0,)), ((), ())), preferred_element_type=f32)


def nt(a, b):
    return lax.dot_general(a, b, (((1,), (1,)), ((), ())), preferred_element_type=f32)


def tn(a, b):
    return lax.dot_general(a, b, (((0,), (0,)), ((), ())), preferred_element_type=f32)


def call(kernel, out_shape, scratch=(), **kw):
    return pl.pallas_call(
        kernel,
        out_shape=out_shape,
        scratch_shapes=list(scratch),
        compiler_params=pltpu.CompilerParams(vmem_limit_bytes=56 * 1024 * 1024),
        **kw,
    )


def struct(shape, dtype):
    return jax.ShapeDtypeStruct(shape, dtype)


def pack_kernel(x_ref, *refs):
    outs, scratch = refs[:4], refs[4]
    levels = x_ref.shape[0]
    rows = levels * HALF_LAT * HALF_LON
    for level in range(levels):
        for lat in range(WIN_LAT):
            slab = x_ref[(level + HALF_LEV) % levels, lat].astype(f32)
            for half in range(2):
                quad = (2 if lat < HALF_LAT else 0) + (1 if half == 0 else 0)
                at = quad * rows + (level * HALF_LAT + lat % HALF_LAT) * HALF_LON
                scratch[at : at + HALF_LON, :] = slab[half * HALF_LON : (half + 1) * HALF_LON, :]
    for quad in range(4):
        outs[quad][...] = scratch[quad * rows : (quad + 1) * rows, :].astype(bf16)


def pack(x):
    levels, _, _, width = x.shape
    rows = levels * HALF_LAT * HALF_LON
    return call(
        pack_kernel,
        [struct((rows, width), bf16)] * 4,
        [pltpu.VMEM((4 * rows, width), f32)],
        name="pack",
    )(x)


def unpack_kernel(q0, q1, q2, q3, out_ref, scratch):
    quads = (q0, q1, q2, q3)
    levels = out_ref.shape[0]
    rows = levels * HALF_LAT * HALF_LON
    for quad in range(4):
        scratch[quad * rows : (quad + 1) * rows, :] = quads[quad][...].astype(f32)
    for level in range(levels):
        for lat in range(WIN_LAT):
            parts = []
            for half in range(2):
                quad = (2 if lat < HALF_LAT else 0) + (1 if half == 0 else 0)
                at = quad * rows + (level * HALF_LAT + lat % HALF_LAT) * HALF_LON
                parts.append(scratch[at : at + HALF_LON, :])
            out_ref[(level + HALF_LEV) % levels, lat] = jnp.concatenate(parts, 0).astype(bf16)


def unpack(quads, shape):
    levels, _, _, width = shape
    rows = levels * HALF_LAT * HALF_LON
    return call(
        unpack_kernel,
        struct(shape, bf16),
        [pltpu.VMEM((4 * rows, width), f32)],
        name="unpack",
    )(*quads)


def coordinates():
    n = np.arange(WINDOW)
    quad, r = n // QUAD, n % QUAD
    lev = r // (HALF_LAT * HALF_LON)
    lat = (quad // 2) * HALF_LAT + r // HALF_LON % HALF_LAT
    lon = (quad % 2) * HALF_LON + r % HALF_LON
    return np.stack([lev, lat, lon]).astype(np.int32)


def table_kernel(pb_ref, col_ref, row_ref, id_col_ref, id_row_ref, out_ref):
    windows = id_col_ref.shape[0]
    bases = (WIN_LEV - 1, 2 * WIN_LEV - 1 + WIN_LAT - 1, 2 * WIN_LEV + 2 * WIN_LAT - 2 + WIN_LON - 1)
    extents = (WIN_LEV, WIN_LAT, WIN_LON)
    block = 8

    def step(b, carry):
        at = pl.multiple_of(b * block, block)
        sums = [None] * HEADS
        for axis in range(3):
            diff = row_ref[axis : axis + 1, :] - col_ref[axis, pl.ds(at, block), :]
            parts = [jnp.zeros((block, WINDOW), f32)] * HEADS
            for offset in range(1 - extents[axis], extents[axis]):
                hit = diff == offset
                parts = [
                    jnp.where(hit, pb_ref[h, bases[axis] + offset], parts[h]) for h in range(HEADS)
                ]
            sums = parts if axis == 0 else [s + p for s, p in zip(sums, parts)]
        for w in range(windows):
            allowed = id_col_ref[w, pl.ds(at, block), :] == id_row_ref[w]
            for h in range(HEADS):
                out_ref[w * HEADS + h, pl.ds(at, block), :] = jnp.where(
                    allowed, sums[h], masked_value
                )
        return carry

    lax.fori_loop(0, WINDOW // block, step, 0)


def score_table(position_bias, mask_ids):
    levels = mask_ids.shape[0]
    windows = levels // WIN_LEV
    ids = mask_ids.reshape(windows, WIN_LEV, 2, HALF_LAT, 2, HALF_LON)
    ids = ids.transpose(0, 2, 4, 1, 3, 5).reshape(windows, WINDOW)
    coords = coordinates()
    vmem = pl.BlockSpec(memory_space=pltpu.VMEM)
    return call(
        table_kernel,
        struct((windows * HEADS, WINDOW, WINDOW), f32),
        in_specs=[pl.BlockSpec(memory_space=pltpu.SMEM), vmem, vmem, vmem, vmem],
        name="table",
    )(
        position_bias,
        jnp.asarray(coords[:, :, None]),
        jnp.asarray(coords),
        ids[:, :, None],
        ids[:, None, :],
    )


def gather_rows(quads, scratch):
    windows = scratch.shape[0] // WINDOW
    for quad in range(4):
        piece = quads[quad][...].astype(f32)
        for w in range(windows):
            at = w * WINDOW + quad * QUAD
            scratch[at : at + QUAD, :] = piece[w * QUAD : (w + 1) * QUAD, :]


def scatter_rows(scratch, outs):
    windows = scratch.shape[0] // WINDOW
    for quad in range(4):
        pieces = [
            scratch[w * WINDOW + quad * QUAD : w * WINDOW + (quad + 1) * QUAD, :]
            for w in range(windows)
        ]
        outs[quad][...] = jnp.concatenate(pieces, 0).astype(bf16)


def forward_kernel(
    x0, x1, x2, x3, table, gain, w_qkv, qkv_down, qkv_up, w_proj, proj_down, proj_up,
    o0, o1, o2, o3, unit_ref, inv_ref, normed_ref, low_ref, qkv_ref, probs_ref, attn_ref, low_proj_ref,
    scratch,
):
    gather_rows((x0, x1, x2, x3), scratch)
    width = scratch.shape[1]
    windows = scratch.shape[0] // WINDOW
    head = width // HEADS
    pair = 2 * head
    rows = scratch[...]
    average = jnp.mean(rows, axis=-1, keepdims=True)
    centered = rows - average
    variance = jnp.mean(centered * centered, axis=-1, keepdims=True)
    inv_std = lax.rsqrt(variance + epsilon)
    unit = centered * inv_std
    normed = (unit * gain[...]).astype(bf16)
    unit_ref[...] = unit
    inv_ref[...] = inv_std
    normed_ref[...] = normed
    low = nt(normed, qkv_down[...]).astype(bf16)
    low_ref[...] = low
    qkv_ref[...] = (nn(normed, w_qkv[...]) + nn(low, qkv_up[...])).astype(bf16)
    scale = 1.0 / math.sqrt(head)
    lane = lax.broadcasted_iota(jnp.int32, (WINDOW, pair), 1)
    for w in range(windows):
        at = slice(w * WINDOW, (w + 1) * WINDOW)
        for p in range(HEADS // 2):
            query = qkv_ref[at, p * pair : (p + 1) * pair]
            keys = qkv_ref[at, width + p * pair : width + (p + 1) * pair]
            values = qkv_ref[at, 2 * width + p * pair : 2 * width + (p + 1) * pair]
            mixed = []
            for h in range(2):
                mine = (lane < head) if h == 0 else (lane >= head)
                index = w * HEADS + 2 * p + h
                scores = nt(keys, jnp.where(mine, query, 0)) * scale + table[index]
                top = jnp.max(scores, axis=0, keepdims=True)
                terms = jnp.exp(scores - top)
                probs = terms * (1.0 / jnp.sum(terms, axis=0, keepdims=True))
                probs_ref[index] = probs
                mixed.append(tn(probs.astype(bf16), values))
            attn_ref[at, p * pair : (p + 1) * pair] = jnp.where(
                lane < head, mixed[0], mixed[1]
            ).astype(bf16)
    attn = attn_ref[...]
    low_proj = nt(attn, proj_down[...]).astype(bf16)
    low_proj_ref[...] = low_proj
    scratch[...] = scratch[...] + nn(attn, w_proj[...]) + nn(low_proj, proj_up[...])
    scatter_rows(scratch, (o0, o1, o2, o3))


def backward_kernel(
    g0, g1, g2, g3, normed_ref, low_ref, qkv_ref, probs_ref, attn_ref, low_proj_ref,
    qkv_up, w_proj, proj_down, proj_up,
    grad_ref, d_qkv_ref, d_low_ref, raw_ref,
):
    gather_rows((g0, g1, g2, g3), grad_ref)
    width = grad_ref.shape[1]
    windows = grad_ref.shape[0] // WINDOW
    head = width // HEADS
    pair = 2 * head
    scale = 1.0 / math.sqrt(head)
    grad = grad_ref[...].astype(bf16)
    d_low_proj = nt(grad, proj_up[...]).astype(bf16)
    d_attn = (nt(grad, w_proj[...]) + nn(d_low_proj, proj_down[...])).astype(bf16)
    lane = lax.broadcasted_iota(jnp.int32, (WINDOW, pair), 1)
    for w in range(windows):
        at = slice(w * WINDOW, (w + 1) * WINDOW)
        for p in range(HEADS // 2):
            cols = [slice(s * width + p * pair, s * width + (p + 1) * pair) for s in range(3)]
            query = qkv_ref[at, cols[0]]
            keys = qkv_ref[at, cols[1]]
            values = qkv_ref[at, cols[2]]
            d_out = d_attn[at, p * pair : (p + 1) * pair]
            d_q, d_k, d_v = [], [], []
            for h in range(2):
                mine = (lane < head) if h == 0 else (lane >= head)
                probs = probs_ref[w * HEADS + 2 * p + h]
                d_probs = nt(values, jnp.where(mine, d_out, 0))
                inner = jnp.sum(d_probs * probs, axis=0, keepdims=True)
                d_scores = (probs * (d_probs - inner) * scale).astype(bf16)
                d_v.append(nn(probs.astype(bf16), d_out))
                d_k.append(nn(d_scores, query))
                d_q.append(tn(d_scores, keys))
            for s, parts in enumerate((d_q, d_k, d_v)):
                d_qkv_ref[at, cols[s]] = jnp.where(lane < head, parts[0], parts[1]).astype(bf16)
    d_qkv = d_qkv_ref[...]
    d_low = nt(d_qkv, qkv_up[...]).astype(bf16)
    d_low_ref[...] = d_low
    raw_ref[:, 0:width] = tn(d_low, normed_ref[...]).astype(bf16)
    raw_ref[:, width : 4 * width] = tn(low_ref[...], d_qkv).astype(bf16)
    raw_ref[:, 4 * width : 5 * width] = tn(d_low_proj, attn_ref[...]).astype(bf16)
    raw_ref[:, 5 * width : 6 * width] = tn(low_proj_ref[...], grad).astype(bf16)


def norm_kernel(
    grad_ref, d_qkv_ref, d_low_ref, unit_ref, inv_ref, gain, w_qkv, qkv_down, o0, o1, o2, o3, scratch
):
    d_normed = nt(d_qkv_ref[...], w_qkv[...]) + nn(d_low_ref[...], qkv_down[...])
    d_unit = d_normed * gain[...]
    unit = unit_ref[...]
    back = inv_ref[...] * (
        d_unit
        - jnp.mean(d_unit, axis=-1, keepdims=True)
        - unit * jnp.mean(d_unit * unit, axis=-1, keepdims=True)
    )
    scratch[...] = grad_ref[...] + back
    scatter_rows(scratch, (o0, o1, o2, o3))


def step_pairs(mesh_shape, lon_by, lat_by):
    lons, lats = mesh_shape
    return [
        (i * lats + j, (i + lon_by) % lons * lats + (j + lat_by) % lats)
        for i in range(lons)
        for j in range(lats)
    ]


def exchange(quads, sizes, by):
    axes = ("lon", "lat")
    far = lax.ppermute(quads[3], axes, step_pairs(sizes, by, by))
    side = lax.ppermute(quads[2], axes, step_pairs(sizes, 0, by))
    near = lax.ppermute(quads[1], axes, step_pairs(sizes, by, 0))
    return [quads[0], near, side, far]


def sum_over(raw, sizes):
    total = None
    for axis, length in (("lon", sizes[0]), ("lat", sizes[1])):
        bit = 1
        while bit < length:
            if total is not None:
                raw = total.astype(bf16)
            other = lax.ppermute(raw, axis, [(i, i ^ bit) for i in range(length)])
            total = raw.astype(f32) + other.astype(f32)
            bit *= 2
    return raw.astype(f32) if total is None else total


def on_device(sizes):
    def body(
        latent, cotangent, mask_ids, position_bias, norm_gain,
        w_qkv, qkv_down, qkv_up, w_proj, proj_down, proj_up,
    ):
        levels, lat_rows, lon_cols, width = latent.shape
        assert (lat_rows, lon_cols) == (WIN_LAT, WIN_LON)
        windows = levels // WIN_LEV
        total = windows * WINDOW
        rank = qkv_down.shape[0]
        quarter = struct((windows * QUAD, width), bf16)
        gain = norm_gain[None, :]
        x_quads = exchange(pack(latent), sizes, -1)
        g_quads = exchange(pack(cotangent), sizes, -1)
        table = score_table(position_bias, mask_ids)
        (
            o0, o1, o2, o3, unit, inv_std, normed, low, qkv, probs, attn, low_proj,
        ) = call(
            forward_kernel,
            [quarter] * 4
            + [
                struct((total, width), f32),
                struct((total, 1), f32),
                struct((total, width), bf16),
                struct((total, rank), bf16),
                struct((total, 3 * width), bf16),
                struct((windows * HEADS, WINDOW, WINDOW), f32),
                struct((total, width), bf16),
                struct((total, rank), bf16),
            ],
            [pltpu.VMEM((total, width), f32)],
            name="forward",
        )(*x_quads, table, gain, w_qkv, qkv_down, qkv_up, w_proj, proj_down, proj_up)
        out_quads = exchange((o0, o1, o2, o3), sizes, 1)
        grad, d_qkv, d_low, raw = call(
            backward_kernel,
            [
                struct((total, width), f32),
                struct((total, 3 * width), bf16),
                struct((total, rank), bf16),
                struct((rank, 6 * width), bf16),
            ],
            name="backward",
        )(*g_quads, normed, low, qkv, probs, attn, low_proj, qkv_up, w_proj, proj_down, proj_up)
        sums = sum_over(raw, sizes)
        back = call(
            norm_kernel,
            [quarter] * 4,
            [pltpu.VMEM((total, width), f32)],
            name="norm_back",
        )(grad, d_qkv, d_low, unit, inv_std, gain, w_qkv, qkv_down)
        back_quads = exchange(back, sizes, 1)
        output = unpack(out_quads, latent.shape)
        latent_grad = unpack(back_quads, latent.shape)
        grad_scale = 1.0 / math.sqrt(levels * lat_rows * lon_cols * sizes[0] * sizes[1])
        sums = sums * grad_scale
        return (
            output,
            latent_grad,
            sums[:, 0:width],
            sums[:, width : 4 * width],
            sums[:, 4 * width : 5 * width],
            sums[:, 5 * width : 6 * width],
        )

    return body


def solution(mesh):
    block = P("runs", "lat", "lon", None)
    sizes = (mesh.shape["lon"], mesh.shape["lat"])
    return jax.shard_map(
        on_device(sizes),
        mesh=mesh,
        in_specs=(block, block, P("runs", "lat", "lon")) + (P(),) * 8,
        out_specs=(block, block) + (P("runs", None),) * 4,
        check_vma=False,
    )
```

```python
import functools
import math

import jax
import jax.numpy as jnp
import numpy as np
from jax import lax
from jax.experimental import pallas as pl
from jax.experimental.pallas import tpu as pltpu
from jax.sharding import PartitionSpec as P

HEADS = 8
WIN_LEV = 2
WIN_LAT = 6
WIN_LON = 12
HALF_LAT = WIN_LAT // 2
HALF_LON = WIN_LON // 2
HALF_LEV = WIN_LEV // 2
WINDOW = WIN_LEV * WIN_LAT * WIN_LON

epsilon = 1e-05
masked_value = -1e30
f32 = jnp.float32
bf16 = jnp.bfloat16


def nn(a, b):
    return lax.dot_general(a, b, (((1,), (0,)), ((), ())), preferred_element_type=f32)


def nt(a, b):
    return lax.dot_general(a, b, (((1,), (1,)), ((), ())), preferred_element_type=f32)


def tn(a, b):
    return lax.dot_general(a, b, (((0,), (0,)), ((), ())), preferred_element_type=f32)


def call(kernel, out_shape, scratch=(), vmem=16, **kw):
    return pl.pallas_call(
        kernel,
        out_shape=out_shape,
        scratch_shapes=list(scratch),
        compiler_params=pltpu.CompilerParams(vmem_limit_bytes=vmem * 1024 * 1024),
        **kw,
    )


def in_hbm(array):
    return pltpu.with_memory_space_constraint(array, pltpu.HBM)


def struct(shape, dtype):
    return jax.ShapeDtypeStruct(shape, dtype)


ANY = pl.BlockSpec(memory_space=pl.ANY)
HBM = pl.BlockSpec(memory_space=pltpu.HBM)
VMEM = pl.BlockSpec(memory_space=pltpu.VMEM)


def corner(ref, quad):
    lat = 0 if quad >= 2 else HALF_LAT
    lon = 0 if quad % 2 else HALF_LON
    return ref.at[lat : lat + HALF_LAT, lon : lon + HALF_LON]


def run_copies(pairs, sems):
    copies = [pltpu.make_async_copy(src, dst, sems.at[i]) for i, (src, dst) in enumerate(pairs)]
    for copy in copies:
        copy.start()
    return copies


def pack_kernel(x_ref, g_ref, *refs):
    outs, sems = refs[:8], refs[8]
    pairs = [(corner(x_ref, q), outs[q]) for q in range(4)]
    pairs += [(corner(g_ref, q), outs[4 + q]) for q in range(4)]
    for copy in run_copies(pairs, sems):
        copy.wait()


def pack(x, g):
    _, _, levels, width = x.shape
    quads = call(
        pack_kernel,
        [struct((HALF_LAT, HALF_LON, levels, width), bf16)] * 8,
        [pltpu.SemaphoreType.DMA((8,))],
        vmem=2,
        in_specs=[HBM] * 2,
        out_specs=[ANY] * 8,
        name="pack",
    )(in_hbm(x), in_hbm(g))
    return quads[:4], quads[4:]


def unpack_kernel(q0, q1, q2, q3, out_ref, sems):
    quads = (q0, q1, q2, q3)
    for copy in run_copies([(quads[q], corner(out_ref, q)) for q in range(4)], sems):
        copy.wait()


def unpack(quads, shape):
    return call(
        unpack_kernel,
        struct(shape, bf16),
        [pltpu.SemaphoreType.DMA((4,))],
        vmem=2,
        in_specs=[ANY] * 4,
        out_specs=ANY,
        name="unpack",
    )(*quads)


AXES = (WIN_LEV, WIN_LAT, WIN_LON)
PLACES = sum(AXES)
SPLITS = 3
MARK = SPLITS * PLACES
LANES = 128


def score_constants():
    n = np.arange(WINDOW)
    lev, r = n // (WINDOW // WIN_LEV), n % (WINDOW // WIN_LEV)
    quad, s = r // (HALF_LAT * HALF_LON), r % (HALF_LAT * HALF_LON)
    lat = (quad // 2) * HALF_LAT + s // HALF_LON
    lon = (quad % 2) * HALF_LON + s % HALF_LON
    starts = (0, WIN_LEV, WIN_LEV + WIN_LAT)
    place = np.zeros((WINDOW, PLACES), np.float32)
    for start, where in zip(starts, (lev, lat, lon)):
        place[n, start + where] = 1
    axis_of = np.repeat(np.arange(3), AXES)
    spot = np.concatenate([np.arange(extent) for extent in AXES])
    bases = (WIN_LEV - 1, 2 * WIN_LEV - 1 + WIN_LAT - 1, 2 * WIN_LEV + 2 * WIN_LAT - 2 + WIN_LON - 1)
    column = np.full((PLACES, HEADS, LANES), -1, np.int32)
    for key in range(PLACES):
        for query in range(PLACES):
            if axis_of[key] == axis_of[query]:
                at = bases[axis_of[key]] + spot[query] - spot[key]
                for part in range(SPLITS):
                    column[key, :, part * PLACES + query] = at
    spread = np.zeros((SPLITS, HEADS, HEADS, LANES), np.float32)
    for part in range(SPLITS):
        for h in range(HEADS):
            spread[part, h, h, part * PLACES : (part + 1) * PLACES] = 1
    query_side = np.zeros((WINDOW, LANES), np.float32)
    query_side[:, :MARK] = np.tile(place, (1, SPLITS))
    first = lev == 0
    lat_of = place[first][:, WIN_LEV : WIN_LEV + WIN_LAT]
    lon_of = place[first][:, WIN_LEV + WIN_LAT :]
    return (
        jnp.asarray(column.reshape(PLACES, HEADS * LANES)),
        jnp.asarray(spread.reshape(SPLITS, HEADS, HEADS * LANES), bf16),
        jnp.asarray(place, bf16),
        jnp.asarray(query_side, f32),
        jnp.asarray(lat_of, f32),
        jnp.asarray(lon_of, f32),
    )


def table_kernel(*refs, count):
    inputs, refs = refs[: 8 + count], refs[8 + count :]
    key_out, query_out = refs[:2]
    kept, local, sems = refs[2 : 2 + count], refs[2 + count : 10 + count], refs[10 + count]
    copies = run_copies(list(zip(inputs, tuple(local) + tuple(kept))), sems)
    for copy in copies[:8]:
        copy.wait()
    make_columns(*local, key_out, query_out)
    for copy in copies[8:]:
        copy.wait()


def make_columns(
    pb_ref, ids_ref, column_ref, spread_ref, place_ref, query_ref, lat_ref, lon_ref, key_out, query_out
):
    windows = key_out.shape[0]
    rest = pb_ref[...]
    wide = None
    for part in range(SPLITS):
        piece = rest.astype(bf16)
        rest = rest - piece.astype(f32)
        term = tn(piece, spread_ref[part])
        wide = term if wide is None else wide + term
    column = column_ref[...]
    table = jnp.zeros(column.shape, f32)
    for c in range(pb_ref.shape[1]):
        table = jnp.where(column == c, wide[c : c + 1, :], table)
    keys = nn(place_ref[...], table.astype(bf16))
    ids = None
    for lat in range(WIN_LAT):
        term = lat_ref[:, lat : lat + 1] * nt(lon_ref[...], ids_ref[lat].astype(f32))
        ids = term if ids is None else ids + term
    half = WINDOW // WIN_LEV
    key_lane = lax.broadcasted_iota(jnp.int32, (half, HEADS * LANES), 1) % LANES
    query_lane = lax.broadcasted_iota(jnp.int32, (half, LANES), 1)
    for w in range(windows):
        key_rows, query_rows = [], []
        for lev in range(WIN_LEV):
            mine = ids[:, w * WIN_LEV + lev : w * WIN_LEV + lev + 1]
            rows = slice(lev * half, (lev + 1) * half)
            key_rows.append(
                jnp.where(
                    key_lane == MARK,
                    masked_value * mine,
                    jnp.where(key_lane == MARK + 1, masked_value * (1.0 - mine), keys[rows]),
                )
            )
            query_rows.append(
                jnp.where(
                    query_lane == MARK,
                    1.0 - mine,
                    jnp.where(query_lane == MARK + 1, mine, query_ref[rows, :]),
                )
            )
        key_out[w] = jnp.concatenate(key_rows, 0).astype(bf16)
        query_out[w] = jnp.concatenate(query_rows, 0).astype(bf16)


def score_columns(position_bias, mask_ids, weights):
    windows = mask_ids.shape[0] // WIN_LEV
    inputs = (position_bias, mask_ids.transpose(1, 0, 2)) + score_constants()
    return call(
        functools.partial(table_kernel, count=len(weights)),
        [struct((windows, WINDOW, HEADS * LANES), bf16), struct((windows, WINDOW, LANES), bf16)]
        + [struct(w.shape, w.dtype) for w in weights],
        [pltpu.VMEM(x.shape, x.dtype) for x in inputs]
        + [pltpu.SemaphoreType.DMA((len(inputs) + len(weights),))],
        in_specs=[HBM] * (len(inputs) + len(weights)),
        name="table",
    )(*map(in_hbm, inputs), *map(in_hbm, weights))


def slabs(quads):
    _, _, levels, _ = quads[0].shape
    for quad in range(4):
        for lat in range(HALF_LAT):
            for lon in range(HALF_LON):
                yield quads[quad], lat, lon, ((quad * HALF_LAT + lat) * HALF_LON + lon) * levels


def gather_rows(quads, scratch, out_ref):
    levels = quads[0].shape[2]
    tiles, total, _ = scratch.shape
    rows = total // levels
    for ref, lat, lon, at in slabs(quads):
        slab = ref[lat, lon].astype(f32)
        for t in range(tiles):
            scratch[t, at : at + levels, :] = slab[:, t * LANES : (t + 1) * LANES]
    for level in range(levels):
        for t in range(tiles):
            out_ref[level * rows : (level + 1) * rows, t * LANES : (t + 1) * LANES] = scratch[
                t, pl.ds((level + HALF_LEV) % levels, rows, stride=levels), :
            ]


def scatter_rows(value, scratch, outs):
    levels = outs[0].shape[2]
    tiles, total, _ = scratch.shape
    rows = total // levels
    for level in range(levels):
        for t in range(tiles):
            scratch[t, pl.ds((level + HALF_LEV) % levels, rows, stride=levels), :] = value[
                level * rows : (level + 1) * rows, t * LANES : (t + 1) * LANES
            ]
    for ref, lat, lon, at in slabs(outs):
        for t in range(tiles):
            ref[lat, lon, :, t * LANES : (t + 1) * LANES] = scratch[t, at : at + levels, :].astype(bf16)


def forward_kernel(
    x0, x1, x2, x3, key_cols, query_cols, gain, w_qkv, qkv_down, qkv_up, w_proj, proj_down, proj_up,
    o0, o1, o2, o3, unit_ref, inv_ref, normed_ref, low_ref, qkv_ref, probs_ref, attn_ref, low_proj_ref,
    scratch, rows_ref,
):
    gather_rows((x0, x1, x2, x3), scratch, rows_ref)
    total, width = rows_ref.shape
    windows = total // WINDOW
    head = width // HEADS
    pair = 2 * head
    rows = rows_ref[...]
    average = jnp.mean(rows, axis=-1, keepdims=True)
    centered = rows - average
    variance = jnp.mean(centered * centered, axis=-1, keepdims=True)
    inv_std = lax.rsqrt(variance + epsilon)
    unit = centered * inv_std
    normed = (unit * gain[...]).astype(bf16)
    unit_ref[...] = unit
    inv_ref[...] = inv_std
    normed_ref[...] = normed
    low = nt(normed, qkv_down[...]).astype(bf16)
    low_ref[...] = low
    qkv_ref[...] = (nn(normed, w_qkv[...]) + nn(low, qkv_up[...])).astype(bf16)
    scale = 1.0 / math.sqrt(head)
    assert math.frexp(scale)[0] == 0.5
    lane = lax.broadcasted_iota(jnp.int32, (WINDOW, pair), 1)
    for w in range(windows):
        at = slice(w * WINDOW, (w + 1) * WINDOW)
        more = query_cols[w]
        for p in range(HEADS // 2):
            query = qkv_ref[at, p * pair : (p + 1) * pair] * jnp.asarray(scale, bf16)
            keys = qkv_ref[at, width + p * pair : width + (p + 1) * pair]
            values = qkv_ref[at, 2 * width + p * pair : 2 * width + (p + 1) * pair]
            mixed = []
            for h in range(2):
                mine = (lane < head) if h == 0 else (lane >= head)
                number = 2 * p + h
                wide_query = jnp.concatenate([jnp.where(mine, query, 0), more], 1)
                wide_keys = jnp.concatenate(
                    [keys, key_cols[w, :, number * LANES : (number + 1) * LANES]], 1
                )
                scores = nt(wide_keys, wide_query)
                top = jnp.max(scores, axis=0, keepdims=True)
                terms = jnp.exp(scores - top)
                probs = terms * (1.0 / jnp.sum(terms, axis=0, keepdims=True))
                probs_ref[w * HEADS + number] = probs
                mixed.append(tn(probs.astype(bf16), values))
            attn_ref[at, p * pair : (p + 1) * pair] = jnp.where(
                lane < head, mixed[0], mixed[1]
            ).astype(bf16)
    attn = attn_ref[...]
    low_proj = nt(attn, proj_down[...]).astype(bf16)
    low_proj_ref[...] = low_proj
    out = rows_ref[...] + nn(attn, w_proj[...]) + nn(low_proj, proj_up[...])
    scatter_rows(out, scratch, (o0, o1, o2, o3))


def backward_kernel(
    g0, g1, g2, g3, normed_ref, low_ref, qkv_ref, probs_ref, attn_ref, low_proj_ref,
    qkv_up, w_proj, proj_down, proj_up,
    grad_ref, d_qkv_ref, d_low_ref, keep_ref, send_ref, scratch,
):
    gather_rows((g0, g1, g2, g3), scratch, grad_ref)
    width = grad_ref.shape[1]
    windows = grad_ref.shape[0] // WINDOW
    head = width // HEADS
    pair = 2 * head
    scale = 1.0 / math.sqrt(head)
    grad = grad_ref[...].astype(bf16)
    d_low_proj = nt(grad, proj_up[...]).astype(bf16)
    d_attn = (nt(grad, w_proj[...]) + nn(d_low_proj, proj_down[...])).astype(bf16)
    lane = lax.broadcasted_iota(jnp.int32, (WINDOW, pair), 1)
    for w in range(windows):
        at = slice(w * WINDOW, (w + 1) * WINDOW)
        for p in range(HEADS // 2):
            cols = [slice(s * width + p * pair, s * width + (p + 1) * pair) for s in range(3)]
            query = qkv_ref[at, cols[0]]
            keys = qkv_ref[at, cols[1]]
            values = qkv_ref[at, cols[2]]
            d_out = d_attn[at, p * pair : (p + 1) * pair]
            d_q, d_k, d_v = [], [], []
            for h in range(2):
                mine = (lane < head) if h == 0 else (lane >= head)
                probs = probs_ref[w * HEADS + 2 * p + h]
                d_probs = nt(values, jnp.where(mine, d_out, 0))
                inner = jnp.sum(d_probs * probs, axis=0, keepdims=True)
                d_scores = (probs * (d_probs - inner) * scale).astype(bf16)
                d_v.append(nn(probs.astype(bf16), d_out))
                d_k.append(nn(d_scores, query))
                d_q.append(tn(d_scores, keys))
            for s, parts in enumerate((d_q, d_k, d_v)):
                d_qkv_ref[at, cols[s]] = jnp.where(lane < head, parts[0], parts[1]).astype(bf16)
    d_qkv = d_qkv_ref[...]
    d_low = nt(d_qkv, qkv_up[...]).astype(bf16)
    d_low_ref[...] = d_low
    raw = jnp.concatenate(
        [
            tn(d_low, normed_ref[...]),
            tn(low_ref[...], d_qkv),
            tn(d_low_proj, attn_ref[...]),
            tn(low_proj_ref[...], grad),
        ],
        1,
    )
    half = keep_ref.shape[1]
    odd = lax.axis_index("lon") % 2

    @pl.when(odd == 0)
    def _():
        keep_ref[...] = raw[:, :half]
        send_ref[...] = raw[:, half:]

    @pl.when(odd == 1)
    def _():
        keep_ref[...] = raw[:, half:]
        send_ref[...] = raw[:, :half]


def norm_kernel(
    grad_ref, d_qkv_ref, d_low_ref, unit_ref, inv_ref, gain, w_qkv, qkv_down, o0, o1, o2, o3, scratch
):
    d_normed = nt(d_qkv_ref[...], w_qkv[...]) + nn(d_low_ref[...], qkv_down[...])
    d_unit = d_normed * gain[...]
    unit = unit_ref[...]
    back = inv_ref[...] * (
        d_unit
        - jnp.mean(d_unit, axis=-1, keepdims=True)
        - unit * jnp.mean(d_unit * unit, axis=-1, keepdims=True)
    )
    scatter_rows(grad_ref[...] + back, scratch, (o0, o1, o2, o3))


def finish_kernel(a_ref, b_ref, *outs, scale):
    total = (a_ref[...].astype(f32) + b_ref[...].astype(f32)) * scale
    start = 0
    for out in outs:
        stop = start + out.shape[1]
        out[...] = total[:, start:stop]
        start = stop


def step_pairs(mesh_shape, lon_by, lat_by):
    lons, lats = mesh_shape
    return [
        (i * lats + j, (i + lon_by) % lons * lats + (j + lat_by) % lats)
        for i in range(lons)
        for j in range(lats)
    ]


def exchange(quads, sizes, by):
    axes = ("lon", "lat")
    near = lax.ppermute(quads[1], axes, step_pairs(sizes, by, 0))
    side = lax.ppermute(quads[2], axes, step_pairs(sizes, 0, by))
    far = lax.ppermute(quads[3], axes, step_pairs(sizes, by, by))
    return [quads[0], near, side, far]


def swap(value, axis, length, bit):
    return lax.ppermute(value, axis, [(i, i ^ bit) for i in range(length)])


def sum_over(keep, send, sizes):
    lons, lats = sizes
    total = keep + swap(send, "lon", lons, 1)
    steps = [("lon", lons, bit) for bit in powers(2, lons)]
    steps += [("lat", lats, bit) for bit in powers(1, lats)]
    for axis, length, bit in steps:
        raw = total.astype(bf16)
        other = swap(raw, axis, length, bit)
        total = raw.astype(f32) + other.astype(f32)
    return total, swap(total, "lon", lons, 1)


def powers(bit, length):
    while bit < length:
        yield bit
        bit *= 2


def finish_kernel(mine_ref, other_ref, *outs, scale):
    half = mine_ref.shape[1]
    odd = lax.axis_index("lon") % 2

    def write(first, second):
        start = 0
        for out in outs:
            stop = start + out.shape[1]
            if start < half:
                cut = min(stop, half)
                out[:, : cut - start] = first[:, start:cut] * scale
            if stop > half:
                cut = max(start, half)
                out[:, cut - start :] = second[:, cut - half : stop - half] * scale
            start = stop

    @pl.when(odd == 0)
    def _():
        write(mine_ref, other_ref)

    @pl.when(odd == 1)
    def _():
        write(other_ref, mine_ref)


def on_device(sizes):
    def layer(
        latent, cotangent, mask_ids, position_bias, norm_gain,
        w_qkv, qkv_down, qkv_up, w_proj, proj_down, proj_up,
    ):
        levels, lat_rows, lon_cols, width = latent.shape
        assert (lat_rows, lon_cols) == (WIN_LAT, WIN_LON)
        windows = levels // WIN_LEV
        total = windows * WINDOW
        rank = qkv_down.shape[0]
        quarter = struct((HALF_LAT, HALF_LON, levels, width), bf16)
        columns = pltpu.VMEM((width // LANES, total, LANES), f32)
        x_quads, g_quads = pack(latent.transpose(1, 2, 0, 3), cotangent.transpose(1, 2, 0, 3))
        x_quads = exchange(x_quads, sizes, -1)
        g_quads = exchange(g_quads, sizes, -1)
        key_cols, query_cols, *weights = score_columns(
            position_bias,
            mask_ids,
            (norm_gain[None, :], w_qkv, qkv_down, qkv_up, w_proj, proj_down, proj_up),
        )
        gain, w_qkv, qkv_down, qkv_up, w_proj, proj_down, proj_up = weights
        (
            o0, o1, o2, o3, unit, inv_std, normed, low, qkv, probs, attn, low_proj,
        ) = call(
            forward_kernel,
            [quarter] * 4
            + [
                struct((total, width), f32),
                struct((total, 1), f32),
                struct((total, width), bf16),
                struct((total, rank), bf16),
                struct((total, 3 * width), bf16),
                struct((windows * HEADS, WINDOW, WINDOW), f32),
                struct((total, width), bf16),
                struct((total, rank), bf16),
            ],
            [columns, pltpu.VMEM((total, width), f32)],
            name="forward",
        )(*x_quads, key_cols, query_cols, *weights)
        out_quads = exchange((o0, o1, o2, o3), sizes, 1)
        grad, d_qkv, d_low, keep, send = call(
            backward_kernel,
            [
                struct((total, width), f32),
                struct((total, 3 * width), bf16),
                struct((total, rank), bf16),
                struct((rank, 3 * width), f32),
                struct((rank, 3 * width), f32),
            ],
            [columns],
            name="backward",
        )(*g_quads, normed, low, qkv, probs, attn, low_proj, qkv_up, w_proj, proj_down, proj_up)
        sums = sum_over(keep, send, sizes)
        back = call(norm_kernel, [quarter] * 4, [columns], name="norm_back")(
            grad, d_qkv, d_low, unit, inv_std, gain, w_qkv, qkv_down
        )
        back_quads = exchange(back, sizes, 1)
        shape = (lat_rows, lon_cols, levels, width)
        output = unpack(out_quads, shape).transpose(2, 0, 1, 3)
        latent_grad = unpack(back_quads, shape).transpose(2, 0, 1, 3)
        grad_scale = 1.0 / math.sqrt(levels * lat_rows * lon_cols * sizes[0] * sizes[1])
        down, up, down_proj, up_proj = call(
            functools.partial(finish_kernel, scale=grad_scale),
            [struct((rank, n * width), f32) for n in (1, 3, 1, 1)],
            vmem=2,
            name="finish",
        )(*sums)
        return (output, latent_grad, down, up, down_proj, up_proj)

    return layer


def solution(mesh):
    block = P("runs", "lat", "lon", None)
    sizes = (mesh.shape["lon"], mesh.shape["lat"])
    return jax.shard_map(
        on_device(sizes),
        mesh=mesh,
        in_specs=(block, block, P("runs", "lat", "lon")) + (P(),) * 8,
        out_specs=(block, block) + (P("runs", None),) * 4,
        check_vma=False,
    )
```

```python
import functools
import math

import jax
import jax.numpy as jnp
import numpy as np
from jax import lax
from jax.experimental import pallas as pl
from jax.experimental.pallas import tpu as pltpu
from jax.sharding import PartitionSpec as P

HEADS = 8
WIN_LEV = 2
WIN_LAT = 6
WIN_LON = 12
HALF_LAT = WIN_LAT // 2
HALF_LON = WIN_LON // 2
HALF_LEV = WIN_LEV // 2
WINDOW = WIN_LEV * WIN_LAT * WIN_LON


epsilon = 1e-05
masked_value = -1e30
f32 = jnp.float32
bf16 = jnp.bfloat16


def nn(a, b):
    return lax.dot_general(a, b, (((1,), (0,)), ((), ())), preferred_element_type=f32)


def nt(a, b):
    return lax.dot_general(a, b, (((1,), (1,)), ((), ())), preferred_element_type=f32)


def tn(a, b):
    return lax.dot_general(a, b, (((0,), (0,)), ((), ())), preferred_element_type=f32)


def call(kernel, out_shape, scratch=(), vmem=16, **kw):
    return pl.pallas_call(
        kernel,
        out_shape=out_shape,
        scratch_shapes=list(scratch),
        compiler_params=pltpu.CompilerParams(vmem_limit_bytes=vmem * 1024 * 1024),
        **kw,
    )


def in_hbm(array):
    return pltpu.with_memory_space_constraint(array, pltpu.HBM)


def struct(shape, dtype):
    return jax.ShapeDtypeStruct(shape, dtype)


ANY = pl.BlockSpec(memory_space=pl.ANY)
HBM = pl.BlockSpec(memory_space=pltpu.HBM)
VMEM = pl.BlockSpec(memory_space=pltpu.VMEM)


def corner(ref, quad):
    lat = 0 if quad >= 2 else HALF_LAT
    lon = 0 if quad % 2 else HALF_LON
    return ref.at[lat : lat + HALF_LAT, lon : lon + HALF_LON]


def run_copies(pairs, sems):
    copies = [pltpu.make_async_copy(src, dst, sems.at[i]) for i, (src, dst) in enumerate(pairs)]
    for copy in copies:
        copy.start()
    return copies


def pack_kernel(x_ref, g_ref, *refs):
    outs, sems = refs[:8], refs[8]
    pairs = [(corner(x_ref, q), outs[q]) for q in range(4)]
    pairs += [(corner(g_ref, q), outs[4 + q]) for q in range(4)]
    for copy in run_copies(pairs, sems):
        copy.wait()


def pack(x, g):
    _, _, levels, width = x.shape
    quads = call(
        pack_kernel,
        [struct((HALF_LAT, HALF_LON, levels, width), bf16)] * 8,
        [pltpu.SemaphoreType.DMA((8,))],
        vmem=2,
        in_specs=[HBM] * 2,
        out_specs=[ANY] * 8,
        name="pack",
    )(in_hbm(x), in_hbm(g))
    return quads[:4], quads[4:]


JOINED = (1, 2, 3)
APART = tuple(quad for quad in range(1, 4) if quad not in JOINED)


def unpack_kernel(*refs):
    outs, sems = refs[-3:-1], refs[-1]
    pairs = []
    for i, quad in enumerate((0,) + APART):
        for n in range(2):
            pairs.append((refs[2 * i + n], corner(outs[n], quad)))
    for i, quad in enumerate(JOINED):
        for n in range(2):
            pairs.append((refs[2 + 2 * len(APART) + i].at[n], corner(outs[n], quad)))
    for copy in run_copies(pairs, sems):
        copy.wait()


def unpack(out, back, shape):
    arrays = []
    for quad in (0,) + APART:
        arrays += [out[quad], back[quad]]
    arrays += [back[quad] for quad in JOINED]
    return call(
        unpack_kernel,
        [struct(shape, bf16)] * 2,
        [pltpu.SemaphoreType.DMA((8,))],
        vmem=2,
        in_specs=[ANY] * len(arrays),
        out_specs=[ANY] * 2,
        name="unpack",
    )(*arrays)


AXES = (WIN_LEV, WIN_LAT, WIN_LON)
PLACES = sum(AXES)
SPLITS = 3
MARK = SPLITS * PLACES
LANES = 128


def score_constants():
    n = np.arange(WINDOW)
    lev, r = n // (WINDOW // WIN_LEV), n % (WINDOW // WIN_LEV)
    quad, s = r // (HALF_LAT * HALF_LON), r % (HALF_LAT * HALF_LON)
    lat = (quad // 2) * HALF_LAT + s // HALF_LON
    lon = (quad % 2) * HALF_LON + s % HALF_LON
    starts = (0, WIN_LEV, WIN_LEV + WIN_LAT)
    place = np.zeros((WINDOW, PLACES), np.float32)
    for start, where in zip(starts, (lev, lat, lon)):
        place[n, start + where] = 1
    axis_of = np.repeat(np.arange(3), AXES)
    spot = np.concatenate([np.arange(extent) for extent in AXES])
    bases = (WIN_LEV - 1, 2 * WIN_LEV - 1 + WIN_LAT - 1, 2 * WIN_LEV + 2 * WIN_LAT - 2 + WIN_LON - 1)
    column = np.full((PLACES, HEADS, LANES), -1, np.int32)
    for key in range(PLACES):
        for query in range(PLACES):
            if axis_of[key] == axis_of[query]:
                at = bases[axis_of[key]] + spot[query] - spot[key]
                for part in range(SPLITS):
                    column[key, :, part * PLACES + query] = at
    spread = np.zeros((SPLITS, HEADS, HEADS, LANES), np.float32)
    for part in range(SPLITS):
        for h in range(HEADS):
            spread[part, h, h, part * PLACES : (part + 1) * PLACES] = 1
    query_side = np.zeros((WINDOW, LANES), np.float32)
    query_side[:, :MARK] = np.tile(place, (1, SPLITS))
    first = lev == 0
    lat_of = place[first][:, WIN_LEV : WIN_LEV + WIN_LAT]
    lon_of = place[first][:, WIN_LEV + WIN_LAT :]
    return (
        jnp.asarray(column.reshape(PLACES, HEADS * LANES)),
        jnp.asarray(spread.reshape(SPLITS, HEADS, HEADS * LANES), bf16),
        jnp.asarray(place, bf16),
        jnp.asarray(query_side, f32),
        jnp.asarray(lat_of, f32),
        jnp.asarray(lon_of, f32),
    )


def table_kernel(*refs, count):
    inputs, refs = refs[: 8 + count], refs[8 + count :]
    key_out, query_out = refs[:2]
    kept, local, sems = refs[2 : 2 + count], refs[2 + count : 10 + count], refs[10 + count]
    copies = run_copies(list(zip(inputs, tuple(local) + tuple(kept))), sems)
    for copy in copies[:8]:
        copy.wait()
    make_columns(*local, key_out, query_out)
    for copy in copies[8:]:
        copy.wait()


def make_columns(
    pb_ref, ids_ref, column_ref, spread_ref, place_ref, query_ref, lat_ref, lon_ref, key_out, query_out
):
    windows = key_out.shape[0]
    rest = pb_ref[...]
    wide = None
    for part in range(SPLITS):
        piece = rest.astype(bf16)
        rest = rest - piece.astype(f32)
        term = tn(piece, spread_ref[part])
        wide = term if wide is None else wide + term
    column = column_ref[...]
    table = jnp.zeros(column.shape, f32)
    for c in range(pb_ref.shape[1]):
        table = jnp.where(column == c, wide[c : c + 1, :], table)
    keys = nn(place_ref[...], table.astype(bf16))
    ids = None
    for lat in range(WIN_LAT):
        term = lat_ref[:, lat : lat + 1] * nt(lon_ref[...], ids_ref[lat].astype(f32))
        ids = term if ids is None else ids + term
    half = WINDOW // WIN_LEV
    key_lane = lax.broadcasted_iota(jnp.int32, (half, HEADS * LANES), 1) % LANES
    query_lane = lax.broadcasted_iota(jnp.int32, (half, LANES), 1)
    for w in range(windows):
        key_rows, query_rows = [], []
        for lev in range(WIN_LEV):
            mine = ids[:, w * WIN_LEV + lev : w * WIN_LEV + lev + 1]
            rows = slice(lev * half, (lev + 1) * half)
            key_rows.append(
                jnp.where(
                    key_lane == MARK,
                    masked_value * mine,
                    jnp.where(key_lane == MARK + 1, masked_value * (1.0 - mine), keys[rows]),
                )
            )
            query_rows.append(
                jnp.where(
                    query_lane == MARK,
                    1.0 - mine,
                    jnp.where(query_lane == MARK + 1, mine, query_ref[rows, :]),
                )
            )
        key_out[w] = jnp.concatenate(key_rows, 0).astype(bf16)
        query_out[w] = jnp.concatenate(query_rows, 0).astype(bf16)


def score_columns(position_bias, mask_ids, weights):
    windows = mask_ids.shape[0] // WIN_LEV
    inputs = (position_bias, mask_ids.transpose(1, 0, 2)) + score_constants()
    return call(
        functools.partial(table_kernel, count=len(weights)),
        [struct((windows, WINDOW, HEADS * LANES), bf16), struct((windows, WINDOW, LANES), bf16)]
        + [struct(w.shape, w.dtype) for w in weights],
        [pltpu.VMEM(x.shape, x.dtype) for x in inputs]
        + [pltpu.SemaphoreType.DMA((len(inputs) + len(weights),))],
        in_specs=[HBM] * (len(inputs) + len(weights)),
        name="table",
    )(*map(in_hbm, inputs), *map(in_hbm, weights))


def slabs(quads):
    _, _, levels, _ = quads[0].shape
    for quad in range(4):
        for lat in range(HALF_LAT):
            for lon in range(HALF_LON):
                yield quads[quad], lat, lon, ((quad * HALF_LAT + lat) * HALF_LON + lon) * levels


def gather_rows(quads, scratch, out_ref):
    levels = quads[0].shape[2]
    tiles, total, _ = scratch.shape
    rows = total // levels
    for ref, lat, lon, at in slabs(quads):
        slab = ref[lat, lon].astype(f32)
        for t in range(tiles):
            scratch[t, at : at + levels, :] = slab[:, t * LANES : (t + 1) * LANES]
    for level in range(levels):
        for t in range(tiles):
            out_ref[level * rows : (level + 1) * rows, t * LANES : (t + 1) * LANES] = scratch[
                t, pl.ds((level + HALF_LEV) % levels, rows, stride=levels), :
            ]


def scatter_rows(value, scratch, outs):
    levels = outs[0].shape[2]
    tiles, total, _ = scratch.shape
    rows = total // levels
    for level in range(levels):
        for t in range(tiles):
            scratch[t, pl.ds((level + HALF_LEV) % levels, rows, stride=levels), :] = value[
                level * rows : (level + 1) * rows, t * LANES : (t + 1) * LANES
            ]
    for ref, lat, lon, at in slabs(outs):
        for t in range(tiles):
            ref[lat, lon, :, t * LANES : (t + 1) * LANES] = scratch[t, at : at + levels, :].astype(bf16)


def forward_kernel(
    x0, x1, x2, x3, key_cols, query_cols, gain, w_qkv, qkv_down, qkv_up, w_proj, proj_down, proj_up,
    o0, o1, o2, o3, unit_ref, inv_ref, normed_ref, low_ref, qkv_ref, probs_ref, attn_ref, low_proj_ref,
    scratch, rows_ref,
):
    gather_rows((x0, x1, x2, x3), scratch, rows_ref)
    total, width = rows_ref.shape
    windows = total // WINDOW
    head = width // HEADS
    pair = 2 * head
    rows = rows_ref[...]
    average = jnp.mean(rows, axis=-1, keepdims=True)
    centered = rows - average
    variance = jnp.mean(centered * centered, axis=-1, keepdims=True)
    inv_std = lax.rsqrt(variance + epsilon)
    unit = centered * inv_std
    normed = (unit * gain[...]).astype(bf16)
    unit_ref[...] = unit
    inv_ref[...] = inv_std
    normed_ref[...] = normed
    low = nt(normed, qkv_down[...]).astype(bf16)
    low_ref[...] = low
    qkv_ref[...] = (nn(normed, w_qkv[...]) + nn(low, qkv_up[...])).astype(bf16)
    scale = 1.0 / math.sqrt(head)
    assert math.frexp(scale)[0] == 0.5
    lane = lax.broadcasted_iota(jnp.int32, (WINDOW, pair), 1)
    for w in range(windows):
        at = slice(w * WINDOW, (w + 1) * WINDOW)
        more = query_cols[w]
        for p in range(HEADS // 2):
            query = qkv_ref[at, p * pair : (p + 1) * pair] * jnp.asarray(scale, bf16)
            keys = qkv_ref[at, width + p * pair : width + (p + 1) * pair]
            values = qkv_ref[at, 2 * width + p * pair : 2 * width + (p + 1) * pair]
            mixed = []
            for h in range(2):
                mine = (lane < head) if h == 0 else (lane >= head)
                number = 2 * p + h
                wide_query = jnp.concatenate([jnp.where(mine, query, 0), more], 1)
                wide_keys = jnp.concatenate(
                    [keys, key_cols[w, :, number * LANES : (number + 1) * LANES]], 1
                )
                scores = nt(wide_keys, wide_query)
                top = jnp.max(scores, axis=0, keepdims=True)
                terms = jnp.exp(scores - top)
                probs = terms * (1.0 / jnp.sum(terms, axis=0, keepdims=True))
                probs_ref[w * HEADS + number] = probs
                mixed.append(tn(probs.astype(bf16), values))
            attn_ref[at, p * pair : (p + 1) * pair] = jnp.where(
                lane < head, mixed[0], mixed[1]
            ).astype(bf16)
    attn = attn_ref[...]
    low_proj = nt(attn, proj_down[...]).astype(bf16)
    low_proj_ref[...] = low_proj
    out = rows_ref[...] + nn(attn, w_proj[...]) + nn(low_proj, proj_up[...])
    scatter_rows(out, scratch, (o0, o1, o2, o3))


def backward_kernel(
    g0, g1, g2, g3, normed_ref, low_ref, qkv_ref, probs_ref, attn_ref, low_proj_ref,
    qkv_up, w_proj, proj_down, proj_up,
    grad_ref, d_qkv_ref, d_low_ref, keep_ref, send_ref, scratch,
):
    gather_rows((g0, g1, g2, g3), scratch, grad_ref)
    width = grad_ref.shape[1]
    windows = grad_ref.shape[0] // WINDOW
    head = width // HEADS
    pair = 2 * head
    scale = 1.0 / math.sqrt(head)
    grad = grad_ref[...].astype(bf16)
    d_low_proj = nt(grad, proj_up[...]).astype(bf16)
    d_attn = (nt(grad, w_proj[...]) + nn(d_low_proj, proj_down[...])).astype(bf16)
    lane = lax.broadcasted_iota(jnp.int32, (WINDOW, pair), 1)
    for w in range(windows):
        at = slice(w * WINDOW, (w + 1) * WINDOW)
        for p in range(HEADS // 2):
            cols = [slice(s * width + p * pair, s * width + (p + 1) * pair) for s in range(3)]
            query = qkv_ref[at, cols[0]]
            keys = qkv_ref[at, cols[1]]
            values = qkv_ref[at, cols[2]]
            d_out = d_attn[at, p * pair : (p + 1) * pair]
            d_q, d_k, d_v = [], [], []
            for h in range(2):
                mine = (lane < head) if h == 0 else (lane >= head)
                probs = probs_ref[w * HEADS + 2 * p + h]
                d_probs = nt(values, jnp.where(mine, d_out, 0))
                inner = jnp.sum(d_probs * probs, axis=0, keepdims=True)
                d_scores = (probs * (d_probs - inner) * scale).astype(bf16)
                d_v.append(nn(probs.astype(bf16), d_out))
                d_k.append(nn(d_scores, query))
                d_q.append(tn(d_scores, keys))
            for s, parts in enumerate((d_q, d_k, d_v)):
                d_qkv_ref[at, cols[s]] = jnp.where(lane < head, parts[0], parts[1]).astype(bf16)
    d_qkv = d_qkv_ref[...]
    d_low = nt(d_qkv, qkv_up[...]).astype(bf16)
    d_low_ref[...] = d_low
    raw = jnp.concatenate(
        [
            tn(d_low, normed_ref[...]),
            tn(low_ref[...], d_qkv),
            tn(d_low_proj, attn_ref[...]),
            tn(low_proj_ref[...], grad),
        ],
        1,
    )
    half = keep_ref.shape[1]
    odd = lax.axis_index("lon") % 2

    @pl.when(odd == 0)
    def _():
        keep_ref[...] = raw[:, :half]
        send_ref[...] = raw[:, half:]

    @pl.when(odd == 1)
    def _():
        keep_ref[...] = raw[:, half:]
        send_ref[...] = raw[:, :half]


def norm_kernel(*refs):
    grad_ref, d_qkv_ref, d_low_ref, unit_ref, inv_ref, gain, w_qkv, qkv_down = refs[:8]
    outgoing, refs = refs[8 : 8 + len(JOINED)], refs[8 + len(JOINED) :]
    outs, scratch = list(refs[:4]), refs[4]
    copies = []
    if JOINED:
        pairs = [(src, outs[quad].at[0]) for src, quad in zip(outgoing, JOINED)]
        copies = run_copies(pairs, refs[5])
        for quad in JOINED:
            outs[quad] = outs[quad].at[1]
    d_normed = nt(d_qkv_ref[...], w_qkv[...]) + nn(d_low_ref[...], qkv_down[...])
    d_unit = d_normed * gain[...]
    unit = unit_ref[...]
    back = inv_ref[...] * (
        d_unit
        - jnp.mean(d_unit, axis=-1, keepdims=True)
        - unit * jnp.mean(d_unit * unit, axis=-1, keepdims=True)
    )
    scatter_rows(grad_ref[...] + back, scratch, outs)
    for copy in copies:
        copy.wait()


def step_pairs(mesh_shape, lon_by, lat_by):
    lons, lats = mesh_shape
    return [
        (i * lats + j, (i + lon_by) % lons * lats + (j + lat_by) % lats)
        for i in range(lons)
        for j in range(lats)
    ]


def exchange(quads, sizes, by):
    moved = dict(quads)
    for quad in moved:
        if quad:
            pairs = step_pairs(sizes, by * (quad % 2), by * (quad // 2))
            moved[quad] = lax.ppermute(moved[quad], ("lon", "lat"), pairs)
    return moved


def swap(value, axis, length, bit):
    return lax.ppermute(value, axis, [(i, i ^ bit) for i in range(length)])


def sum_over(keep, send, sizes):
    lons, lats = sizes
    total = keep + swap(send, "lon", lons, 1)
    steps = [("lat", lats, bit) for bit in powers(1, lats)]
    steps += [("lon", lons, bit) for bit in powers(2, lons)]
    for axis, length, bit in steps:
        raw = total.astype(bf16)
        other = swap(raw, axis, length, bit)
        total = raw.astype(f32) + other.astype(f32)
    return total, swap(total, "lon", lons, 1)


def powers(bit, length):
    while bit < length:
        yield bit
        bit *= 2


def finish_kernel(mine_ref, other_ref, *outs, scale):
    half = mine_ref.shape[1]
    odd = lax.axis_index("lon") % 2

    def write(first, second):
        start = 0
        for out in outs:
            stop = start + out.shape[1]
            if start < half:
                cut = min(stop, half)
                out[:, : cut - start] = first[:, start:cut] * scale
            if stop > half:
                cut = max(start, half)
                out[:, cut - start :] = second[:, cut - half : stop - half] * scale
            start = stop

    @pl.when(odd == 0)
    def _():
        write(mine_ref, other_ref)

    @pl.when(odd == 1)
    def _():
        write(other_ref, mine_ref)


def on_device(sizes):
    def layer(
        latent, cotangent, mask_ids, position_bias, norm_gain,
        w_qkv, qkv_down, qkv_up, w_proj, proj_down, proj_up,
    ):
        levels, lat_rows, lon_cols, width = latent.shape
        assert (lat_rows, lon_cols) == (WIN_LAT, WIN_LON)
        windows = levels // WIN_LEV
        total = windows * WINDOW
        rank = qkv_down.shape[0]
        quarter = struct((HALF_LAT, HALF_LON, levels, width), bf16)
        columns = pltpu.VMEM((width // LANES, total, LANES), f32)
        x_quads, g_quads = pack(latent.transpose(1, 2, 0, 3), cotangent.transpose(1, 2, 0, 3))
        x_quads = exchange(enumerate(x_quads), sizes, -1).values()
        g_quads = exchange(enumerate(g_quads), sizes, -1).values()
        key_cols, query_cols, *weights = score_columns(
            position_bias,
            mask_ids,
            (norm_gain[None, :], w_qkv, qkv_down, qkv_up, w_proj, proj_down, proj_up),
        )
        gain, w_qkv, qkv_down, qkv_up, w_proj, proj_down, proj_up = weights
        (
            o0, o1, o2, o3, unit, inv_std, normed, low, qkv, probs, attn, low_proj,
        ) = call(
            forward_kernel,
            [quarter] * 4
            + [
                struct((total, width), f32),
                struct((total, 1), f32),
                struct((total, width), bf16),
                struct((total, rank), bf16),
                struct((total, 3 * width), bf16),
                struct((windows * HEADS, WINDOW, WINDOW), f32),
                struct((total, width), bf16),
                struct((total, rank), bf16),
            ],
            [columns, pltpu.VMEM((total, width), f32)],
            name="forward",
        )(*x_quads, key_cols, query_cols, *weights)
        out = exchange({0: o0, **{q: (o1, o2, o3)[q - 1] for q in APART}}, sizes, 1)
        grad, d_qkv, d_low, keep, send = call(
            backward_kernel,
            [
                struct((total, width), f32),
                struct((total, 3 * width), bf16),
                struct((total, rank), bf16),
                struct((rank, 3 * width), f32),
                struct((rank, 3 * width), f32),
            ],
            [columns],
            name="backward",
        )(*g_quads, normed, low, qkv, probs, attn, low_proj, qkv_up, w_proj, proj_down, proj_up)
        sums = sum_over(keep, send, sizes)
        shapes = [quarter] * 4
        for quad in JOINED:
            shapes[quad] = struct((2,) + quarter.shape, bf16)
        back = call(
            norm_kernel,
            shapes,
            [columns] + [pltpu.SemaphoreType.DMA((len(JOINED),))] * bool(JOINED),
            in_specs=[pl.BlockSpec()] * 8 + [ANY] * len(JOINED),
            name="norm_back",
        )(grad, d_qkv, d_low, unit, inv_std, gain, w_qkv, qkv_down, *[(o1, o2, o3)[q - 1] for q in JOINED])
        back = exchange(enumerate(back), sizes, 1)
        output, latent_grad = unpack(out, back, (lat_rows, lon_cols, levels, width))
        output, latent_grad = (x.transpose(2, 0, 1, 3) for x in (output, latent_grad))
        grad_scale = 1.0 / math.sqrt(levels * lat_rows * lon_cols * sizes[0] * sizes[1])
        down, up, down_proj, up_proj = call(
            functools.partial(finish_kernel, scale=grad_scale),
            [struct((rank, n * width), f32) for n in (1, 3, 1, 1)],
            vmem=2,
            name="finish",
        )(*sums)
        return (output, latent_grad, down, up, down_proj, up_proj)

    return layer


def solution(mesh):
    block = P("runs", "lat", "lon", None)
    sizes = (mesh.shape["lon"], mesh.shape["lat"])
    return jax.shard_map(
        on_device(sizes),
        mesh=mesh,
        in_specs=(block, block, P("runs", "lat", "lon")) + (P(),) * 8,
        out_specs=(block, block) + (P("runs", None),) * 4,
        check_vma=False,
    )
```

```python
import functools
import math

import jax
import jax.numpy as jnp
import numpy as np
from jax import lax
from jax.experimental import pallas as pl
from jax.experimental.pallas import tpu as pltpu
from jax.sharding import PartitionSpec as P

HEADS = 8
WIN_LEV = 2
WIN_LAT = 6
WIN_LON = 12
HALF_LAT = WIN_LAT // 2
HALF_LON = WIN_LON // 2
HALF_LEV = WIN_LEV // 2
WINDOW = WIN_LEV * WIN_LAT * WIN_LON


epsilon = 1e-05
masked_value = -1e30
f32 = jnp.float32
bf16 = jnp.bfloat16


def nn(a, b):
    return lax.dot_general(a, b, (((1,), (0,)), ((), ())), preferred_element_type=f32)


def nt(a, b):
    return lax.dot_general(a, b, (((1,), (1,)), ((), ())), preferred_element_type=f32)


def tn(a, b):
    return lax.dot_general(a, b, (((0,), (0,)), ((), ())), preferred_element_type=f32)


def call(kernel, out_shape, scratch=(), vmem=16, **kw):
    return pl.pallas_call(
        kernel,
        out_shape=out_shape,
        scratch_shapes=list(scratch),
        compiler_params=pltpu.CompilerParams(vmem_limit_bytes=vmem * 1024 * 1024),
        **kw,
    )


def in_hbm(array):
    return pltpu.with_memory_space_constraint(array, pltpu.HBM)


def struct(shape, dtype):
    return jax.ShapeDtypeStruct(shape, dtype)


ANY = pl.BlockSpec(memory_space=pl.ANY)
HBM = pl.BlockSpec(memory_space=pltpu.HBM)
VMEM = pl.BlockSpec(memory_space=pltpu.VMEM)


def corner(ref, quad):
    lat = 0 if quad >= 2 else HALF_LAT
    lon = 0 if quad % 2 else HALF_LON
    return ref.at[lat : lat + HALF_LAT, lon : lon + HALF_LON]


def run_copies(pairs, sems):
    copies = [pltpu.make_async_copy(src, dst, sems.at[i]) for i, (src, dst) in enumerate(pairs)]
    for copy in copies:
        copy.start()
    return copies


def pack_kernel(x_ref, g_ref, *refs):
    outs, sems = refs[:8], refs[8]
    pairs = [(corner(x_ref, q), outs[q]) for q in range(4)]
    pairs += [(corner(g_ref, q), outs[4 + q]) for q in range(4)]
    for copy in run_copies(pairs, sems):
        copy.wait()


def pack(x, g):
    _, _, levels, width = x.shape
    quads = call(
        pack_kernel,
        [struct((HALF_LAT, HALF_LON, levels, width), bf16)] * 8,
        [pltpu.SemaphoreType.DMA((8,))],
        vmem=2,
        in_specs=[HBM] * 2,
        out_specs=[ANY] * 8,
        name="pack",
    )(in_hbm(x), in_hbm(g))
    return quads[:4], quads[4:]


JOINED = (1, 2, 3)
APART = tuple(quad for quad in range(1, 4) if quad not in JOINED)


def unpack_kernel(*refs):
    outs, sems = refs[-3:-1], refs[-1]
    pairs = []
    for i, quad in enumerate((0,) + APART):
        for n in range(2):
            pairs.append((refs[2 * i + n], corner(outs[n], quad)))
    for i, quad in enumerate(JOINED):
        for n in range(2):
            pairs.append((refs[2 + 2 * len(APART) + i].at[n], corner(outs[n], quad)))
    for copy in run_copies(pairs, sems):
        copy.wait()


def unpack(out, back, shape):
    arrays = []
    for quad in (0,) + APART:
        arrays += [out[quad], back[quad]]
    arrays += [back[quad] for quad in JOINED]
    return call(
        unpack_kernel,
        [struct(shape, bf16)] * 2,
        [pltpu.SemaphoreType.DMA((8,))],
        vmem=2,
        in_specs=[ANY] * len(arrays),
        out_specs=[ANY] * 2,
        name="unpack",
    )(*arrays)


AXES = (WIN_LEV, WIN_LAT, WIN_LON)
PLACES = sum(AXES)
SPLITS = 3
MARK = SPLITS * PLACES
LANES = 128


def score_constants():
    n = np.arange(WINDOW)
    lev, r = n // (WINDOW // WIN_LEV), n % (WINDOW // WIN_LEV)
    quad, s = r // (HALF_LAT * HALF_LON), r % (HALF_LAT * HALF_LON)
    lat = (quad // 2) * HALF_LAT + s // HALF_LON
    lon = (quad % 2) * HALF_LON + s % HALF_LON
    starts = (0, WIN_LEV, WIN_LEV + WIN_LAT)
    place = np.zeros((WINDOW, PLACES), np.float32)
    for start, where in zip(starts, (lev, lat, lon)):
        place[n, start + where] = 1
    axis_of = np.repeat(np.arange(3), AXES)
    spot = np.concatenate([np.arange(extent) for extent in AXES])
    bases = (WIN_LEV - 1, 2 * WIN_LEV - 1 + WIN_LAT - 1, 2 * WIN_LEV + 2 * WIN_LAT - 2 + WIN_LON - 1)
    column = np.full((PLACES, HEADS, LANES), -1, np.int32)
    for key in range(PLACES):
        for query in range(PLACES):
            if axis_of[key] == axis_of[query]:
                at = bases[axis_of[key]] + spot[query] - spot[key]
                for part in range(SPLITS):
                    column[key, :, part * PLACES + query] = at
    spread = np.zeros((SPLITS, HEADS, HEADS, LANES), np.float32)
    for part in range(SPLITS):
        for h in range(HEADS):
            spread[part, h, h, part * PLACES : (part + 1) * PLACES] = 1
    query_side = np.zeros((WINDOW, LANES), np.float32)
    query_side[:, :MARK] = np.tile(place, (1, SPLITS))
    first = lev == 0
    lat_of = place[first][:, WIN_LEV : WIN_LEV + WIN_LAT]
    lon_of = place[first][:, WIN_LEV + WIN_LAT :]
    return (
        jnp.asarray(column.reshape(PLACES, HEADS * LANES)),
        jnp.asarray(spread.reshape(SPLITS, HEADS, HEADS * LANES), bf16),
        jnp.asarray(place, bf16),
        jnp.asarray(query_side, f32),
        jnp.asarray(lat_of, f32),
        jnp.asarray(lon_of, f32),
    )


def table_kernel(*refs, count):
    inputs, refs = refs[: 8 + count], refs[8 + count :]
    key_out, query_out = refs[:2]
    kept, local, sems = refs[2 : 2 + count], refs[2 + count : 10 + count], refs[10 + count]
    copies = run_copies(list(zip(inputs, tuple(local) + tuple(kept))), sems)
    for copy in copies[:8]:
        copy.wait()
    make_columns(*local, key_out, query_out)
    for copy in copies[8:]:
        copy.wait()


def make_columns(
    pb_ref, ids_ref, column_ref, spread_ref, place_ref, query_ref, lat_ref, lon_ref, key_out, query_out
):
    windows = key_out.shape[0]
    rest = pb_ref[...]
    wide = None
    for part in range(SPLITS):
        piece = rest.astype(bf16)
        rest = rest - piece.astype(f32)
        term = tn(piece, spread_ref[part])
        wide = term if wide is None else wide + term
    column = column_ref[...]
    table = jnp.zeros(column.shape, f32)
    for c in range(pb_ref.shape[1]):
        table = jnp.where(column == c, wide[c : c + 1, :], table)
    keys = nn(place_ref[...], table.astype(bf16))
    ids = None
    for lat in range(WIN_LAT):
        term = lat_ref[:, lat : lat + 1] * nt(lon_ref[...], ids_ref[lat].astype(f32))
        ids = term if ids is None else ids + term
    half = WINDOW // WIN_LEV
    key_lane = lax.broadcasted_iota(jnp.int32, (half, HEADS * LANES), 1) % LANES
    query_lane = lax.broadcasted_iota(jnp.int32, (half, LANES), 1)
    for w in range(windows):
        key_rows, query_rows = [], []
        for lev in range(WIN_LEV):
            mine = ids[:, w * WIN_LEV + lev : w * WIN_LEV + lev + 1]
            rows = slice(lev * half, (lev + 1) * half)
            key_rows.append(
                jnp.where(
                    key_lane == MARK,
                    masked_value * mine,
                    jnp.where(key_lane == MARK + 1, masked_value * (1.0 - mine), keys[rows]),
                )
            )
            query_rows.append(
                jnp.where(
                    query_lane == MARK,
                    1.0 - mine,
                    jnp.where(query_lane == MARK + 1, mine, query_ref[rows, :]),
                )
            )
        key_out[w] = jnp.concatenate(key_rows, 0).astype(bf16)
        query_out[w] = jnp.concatenate(query_rows, 0).astype(bf16)


def score_columns(position_bias, mask_ids, weights):
    windows = mask_ids.shape[0] // WIN_LEV
    inputs = (position_bias, mask_ids.transpose(1, 0, 2)) + score_constants()
    return call(
        functools.partial(table_kernel, count=len(weights)),
        [struct((windows, WINDOW, HEADS * LANES), bf16), struct((windows, WINDOW, LANES), bf16)]
        + [struct(w.shape, w.dtype) for w in weights],
        [pltpu.VMEM(x.shape, x.dtype) for x in inputs]
        + [pltpu.SemaphoreType.DMA((len(inputs) + len(weights),))],
        in_specs=[HBM] * (len(inputs) + len(weights)),
        name="table",
    )(*map(in_hbm, inputs), *map(in_hbm, weights))


def slabs(quads):
    _, _, levels, _ = quads[0].shape
    for quad in range(4):
        for lat in range(HALF_LAT):
            for lon in range(HALF_LON):
                yield quads[quad], lat, lon, ((quad * HALF_LAT + lat) * HALF_LON + lon) * levels


def gather_rows(quads, scratch, out_ref):
    levels = quads[0].shape[2]
    tiles, total, _ = scratch.shape
    rows = total // levels
    for ref, lat, lon, at in slabs(quads):
        slab = ref[lat, lon].astype(f32)
        for t in range(tiles):
            scratch[t, at : at + levels, :] = slab[:, t * LANES : (t + 1) * LANES]
    for level in range(levels):
        for t in range(tiles):
            out_ref[level * rows : (level + 1) * rows, t * LANES : (t + 1) * LANES] = scratch[
                t, pl.ds((level + HALF_LEV) % levels, rows, stride=levels), :
            ]


def scatter_rows(value, scratch, outs):
    levels = outs[0].shape[2]
    tiles, total, _ = scratch.shape
    rows = total // levels
    for level in range(levels):
        for t in range(tiles):
            scratch[t, pl.ds((level + HALF_LEV) % levels, rows, stride=levels), :] = value[
                level * rows : (level + 1) * rows, t * LANES : (t + 1) * LANES
            ]
    for ref, lat, lon, at in slabs(outs):
        for t in range(tiles):
            ref[lat, lon, :, t * LANES : (t + 1) * LANES] = scratch[t, at : at + levels, :].astype(bf16)


def forward_kernel(
    x0, x1, x2, x3, key_cols, query_cols, gain, w_qkv, qkv_down, qkv_up, w_proj, proj_down, proj_up,
    o0, o1, o2, o3, unit_ref, inv_ref, normed_ref, low_ref, qkv_ref, probs_ref, attn_ref, low_proj_ref,
    scratch, rows_ref, scores_ref, rounded_ref,
):
    gather_rows((x0, x1, x2, x3), scratch, rows_ref)
    total, width = rows_ref.shape
    windows = total // WINDOW
    head = width // HEADS
    pair = 2 * head
    rows = rows_ref[...]
    average = jnp.mean(rows, axis=-1, keepdims=True)
    centered = rows - average
    variance = jnp.mean(centered * centered, axis=-1, keepdims=True)
    inv_std = lax.rsqrt(variance + epsilon)
    unit = centered * inv_std
    normed = (unit * gain[...]).astype(bf16)
    unit_ref[...] = unit
    inv_ref[...] = inv_std
    normed_ref[...] = normed
    low = nt(normed, qkv_down[...]).astype(bf16)
    low_ref[...] = low
    qkv_ref[...] = (nn(normed, w_qkv[...]) + nn(low, qkv_up[...])).astype(bf16)
    scale = 1.0 / math.sqrt(head)
    assert math.frexp(scale)[0] == 0.5
    lane = lax.broadcasted_iota(jnp.int32, (WINDOW, pair), 1)
    pairs = [(w, p) for w in range(windows) for p in range(HEADS // 2)]

    def start(w, p):
        at = slice(w * WINDOW, (w + 1) * WINDOW)
        query = qkv_ref[at, p * pair : (p + 1) * pair] * jnp.asarray(scale, bf16)
        keys = qkv_ref[at, width + p * pair : width + (p + 1) * pair]
        for h in range(2):
            mine = (lane < head) if h == 0 else (lane >= head)
            number = 2 * p + h
            wide_query = jnp.concatenate([jnp.where(mine, query, 0), query_cols[w]], 1)
            wide_keys = jnp.concatenate(
                [keys, key_cols[w, :, number * LANES : (number + 1) * LANES]], 1
            )
            scores_ref[w * HEADS + number] = nt(wide_keys, wide_query)

    def middle(w, p):
        for h in range(2):
            index = w * HEADS + 2 * p + h
            scores = scores_ref[index]
            terms = jnp.exp(scores - jnp.max(scores, axis=0, keepdims=True))
            probs = terms * (1.0 / jnp.sum(terms, axis=0, keepdims=True))
            probs_ref[index] = probs
            rounded_ref[index] = probs.astype(bf16)

    def end(w, p):
        at = slice(w * WINDOW, (w + 1) * WINDOW)
        values = qkv_ref[at, 2 * width + p * pair : 2 * width + (p + 1) * pair]
        mixed = [tn(rounded_ref[w * HEADS + 2 * p + h], values) for h in range(2)]
        attn_ref[at, p * pair : (p + 1) * pair] = jnp.where(
            lane < head, mixed[0], mixed[1]
        ).astype(bf16)

    for stage in (start, middle, end):
        for w, p in pairs:
            stage(w, p)
    attn = attn_ref[...]
    low_proj = nt(attn, proj_down[...]).astype(bf16)
    low_proj_ref[...] = low_proj
    out = rows_ref[...] + nn(attn, w_proj[...]) + nn(low_proj, proj_up[...])
    scatter_rows(out, scratch, (o0, o1, o2, o3))


def backward_kernel(
    g0, g1, g2, g3, normed_ref, low_ref, qkv_ref, probs_ref, attn_ref, low_proj_ref,
    qkv_up, w_proj, proj_down, proj_up,
    grad_ref, d_qkv_ref, d_low_ref, keep_ref, send_ref, scratch, probs_grad, scores_grad,
):
    gather_rows((g0, g1, g2, g3), scratch, grad_ref)
    width = grad_ref.shape[1]
    windows = grad_ref.shape[0] // WINDOW
    head = width // HEADS
    pair = 2 * head
    scale = 1.0 / math.sqrt(head)
    grad = grad_ref[...].astype(bf16)
    d_low_proj = nt(grad, proj_up[...]).astype(bf16)
    d_attn = (nt(grad, w_proj[...]) + nn(d_low_proj, proj_down[...])).astype(bf16)
    lane = lax.broadcasted_iota(jnp.int32, (WINDOW, pair), 1)
    pairs = [(w, p) for w in range(windows) for p in range(HEADS // 2)]

    def start(w, p):
        at = slice(w * WINDOW, (w + 1) * WINDOW)
        values = qkv_ref[at, 2 * width + p * pair : 2 * width + (p + 1) * pair]
        scaled = d_attn[at, p * pair : (p + 1) * pair] * jnp.asarray(scale, bf16)
        for h in range(2):
            mine = (lane < head) if h == 0 else (lane >= head)
            probs_grad[w * HEADS + 2 * p + h] = nt(values, jnp.where(mine, scaled, 0))

    def middle(w, p):
        for h in range(2):
            index = w * HEADS + 2 * p + h
            probs = probs_ref[index]
            d_probs = probs_grad[index]
            inner = jnp.sum(d_probs * probs, axis=0, keepdims=True)
            scores_grad[index] = (probs * (d_probs - inner)).astype(bf16)

    def end(w, p):
        at = slice(w * WINDOW, (w + 1) * WINDOW)
        cols = [slice(s * width + p * pair, s * width + (p + 1) * pair) for s in range(3)]
        query = qkv_ref[at, cols[0]]
        keys_t = qkv_ref[at, cols[1]].T
        d_out = d_attn[at, p * pair : (p + 1) * pair]
        d_q, d_k, d_v = [], [], []
        for h in range(2):
            index = w * HEADS + 2 * p + h
            d_scores = scores_grad[index]
            d_v.append(nn(probs_ref[index].astype(bf16), d_out))
            d_k.append(nn(d_scores, query))
            d_q.append(nn(keys_t[h * head : (h + 1) * head], d_scores).astype(bf16))
        d_qkv_ref[at, cols[0]] = jnp.concatenate(d_q, 0).T
        for s, parts in ((1, d_k), (2, d_v)):
            d_qkv_ref[at, cols[s]] = jnp.where(lane < head, parts[0], parts[1]).astype(bf16)

    for i in range(len(pairs) + 2):
        if i < len(pairs):
            start(*pairs[i])
        if 1 <= i <= len(pairs):
            middle(*pairs[i - 1])
        if i >= 2:
            end(*pairs[i - 2])
    d_qkv = d_qkv_ref[...]
    d_low = nt(d_qkv, qkv_up[...]).astype(bf16)
    d_low_ref[...] = d_low
    raw = jnp.concatenate(
        [
            tn(d_low, normed_ref[...]),
            tn(low_ref[...], d_qkv),
            tn(d_low_proj, attn_ref[...]),
            tn(low_proj_ref[...], grad),
        ],
        1,
    )
    half = keep_ref.shape[1]
    odd = lax.axis_index("lon") % 2

    @pl.when(odd == 0)
    def _():
        keep_ref[...] = raw[:, :half]
        send_ref[...] = raw[:, half:]

    @pl.when(odd == 1)
    def _():
        keep_ref[...] = raw[:, half:]
        send_ref[...] = raw[:, :half]


def norm_kernel(*refs):
    grad_ref, d_qkv_ref, d_low_ref, unit_ref, inv_ref, gain, w_qkv, qkv_down = refs[:8]
    outgoing, refs = refs[8 : 8 + len(JOINED)], refs[8 + len(JOINED) :]
    outs, scratch = list(refs[:4]), refs[4]
    copies = []
    if JOINED:
        pairs = [(src, outs[quad].at[0]) for src, quad in zip(outgoing, JOINED)]
        copies = run_copies(pairs, refs[5])
        for quad in JOINED:
            outs[quad] = outs[quad].at[1]
    d_normed = nt(d_qkv_ref[...], w_qkv[...]) + nn(d_low_ref[...], qkv_down[...])
    d_unit = d_normed * gain[...]
    unit = unit_ref[...]
    back = inv_ref[...] * (
        d_unit
        - jnp.mean(d_unit, axis=-1, keepdims=True)
        - unit * jnp.mean(d_unit * unit, axis=-1, keepdims=True)
    )
    scatter_rows(grad_ref[...] + back, scratch, outs)
    for copy in copies:
        copy.wait()


def step_pairs(mesh_shape, lon_by, lat_by):
    lons, lats = mesh_shape
    return [
        (i * lats + j, (i + lon_by) % lons * lats + (j + lat_by) % lats)
        for i in range(lons)
        for j in range(lats)
    ]


def exchange(quads, sizes, by):
    moved = dict(quads)
    for quad in moved:
        if quad:
            pairs = step_pairs(sizes, by * (quad % 2), by * (quad // 2))
            moved[quad] = lax.ppermute(moved[quad], ("lon", "lat"), pairs)
    return moved


def swap(value, axis, length, bit):
    return lax.ppermute(value, axis, [(i, i ^ bit) for i in range(length)])


def sum_over(keep, send, sizes):
    lons, lats = sizes
    total = keep + swap(send, "lon", lons, 1)
    steps = [("lat", lats, bit) for bit in powers(1, lats)]
    steps += [("lon", lons, bit) for bit in powers(2, lons)]
    for axis, length, bit in steps:
        raw = total.astype(bf16)
        other = swap(raw, axis, length, bit)
        total = raw.astype(f32) + other.astype(f32)
    return total, swap(total, "lon", lons, 1)


def powers(bit, length):
    while bit < length:
        yield bit
        bit *= 2


def finish_kernel(mine_ref, other_ref, *outs, scale):
    half = mine_ref.shape[1]
    odd = lax.axis_index("lon") % 2

    def write(first, second):
        start = 0
        for out in outs:
            stop = start + out.shape[1]
            if start < half:
                cut = min(stop, half)
                out[:, : cut - start] = first[:, start:cut] * scale
            if stop > half:
                cut = max(start, half)
                out[:, cut - start :] = second[:, cut - half : stop - half] * scale
            start = stop

    @pl.when(odd == 0)
    def _():
        write(mine_ref, other_ref)

    @pl.when(odd == 1)
    def _():
        write(other_ref, mine_ref)


def on_device(sizes):
    def layer(
        latent, cotangent, mask_ids, position_bias, norm_gain,
        w_qkv, qkv_down, qkv_up, w_proj, proj_down, proj_up,
    ):
        levels, lat_rows, lon_cols, width = latent.shape
        assert (lat_rows, lon_cols) == (WIN_LAT, WIN_LON)
        windows = levels // WIN_LEV
        total = windows * WINDOW
        rank = qkv_down.shape[0]
        quarter = struct((HALF_LAT, HALF_LON, levels, width), bf16)
        columns = pltpu.VMEM((width // LANES, total, LANES), f32)
        x_quads, g_quads = pack(latent.transpose(1, 2, 0, 3), cotangent.transpose(1, 2, 0, 3))
        x_quads = exchange(enumerate(x_quads), sizes, -1).values()
        g_quads = exchange(enumerate(g_quads), sizes, -1).values()
        key_cols, query_cols, *weights = score_columns(
            position_bias,
            mask_ids,
            (norm_gain[None, :], w_qkv, qkv_down, qkv_up, w_proj, proj_down, proj_up),
        )
        gain, w_qkv, qkv_down, qkv_up, w_proj, proj_down, proj_up = weights
        (
            o0, o1, o2, o3, unit, inv_std, normed, low, qkv, probs, attn, low_proj,
        ) = call(
            forward_kernel,
            [quarter] * 4
            + [
                struct((total, width), f32),
                struct((total, 1), f32),
                struct((total, width), bf16),
                struct((total, rank), bf16),
                struct((total, 3 * width), bf16),
                struct((windows * HEADS, WINDOW, WINDOW), f32),
                struct((total, width), bf16),
                struct((total, rank), bf16),
            ],
            [
                columns,
                pltpu.VMEM((total, width), f32),
                pltpu.VMEM((windows * HEADS, WINDOW, WINDOW), f32),
                pltpu.VMEM((windows * HEADS, WINDOW, WINDOW), bf16),
            ],
            name="forward",
        )(*x_quads, key_cols, query_cols, *weights)
        out = exchange({0: o0, **{q: (o1, o2, o3)[q - 1] for q in APART}}, sizes, 1)
        grad, d_qkv, d_low, keep, send = call(
            backward_kernel,
            [
                struct((total, width), f32),
                struct((total, 3 * width), bf16),
                struct((total, rank), bf16),
                struct((rank, 3 * width), f32),
                struct((rank, 3 * width), f32),
            ],
            [
                columns,
                pltpu.VMEM((windows * HEADS, WINDOW, WINDOW), f32),
                pltpu.VMEM((windows * HEADS, WINDOW, WINDOW), bf16),
            ],
            name="backward",
        )(*g_quads, normed, low, qkv, probs, attn, low_proj, qkv_up, w_proj, proj_down, proj_up)
        sums = sum_over(keep, send, sizes)
        shapes = [quarter] * 4
        for quad in JOINED:
            shapes[quad] = struct((2,) + quarter.shape, bf16)
        back = call(
            norm_kernel,
            shapes,
            [columns] + [pltpu.SemaphoreType.DMA((len(JOINED),))] * bool(JOINED),
            in_specs=[pl.BlockSpec()] * 8 + [ANY] * len(JOINED),
            name="norm_back",
        )(grad, d_qkv, d_low, unit, inv_std, gain, w_qkv, qkv_down, *[(o1, o2, o3)[q - 1] for q in JOINED])
        back = exchange(enumerate(back), sizes, 1)
        output, latent_grad = unpack(out, back, (lat_rows, lon_cols, levels, width))
        output, latent_grad = (x.transpose(2, 0, 1, 3) for x in (output, latent_grad))
        grad_scale = 1.0 / math.sqrt(levels * lat_rows * lon_cols * sizes[0] * sizes[1])
        down, up, down_proj, up_proj = call(
            functools.partial(finish_kernel, scale=grad_scale),
            [struct((rank, n * width), f32) for n in (1, 3, 1, 1)],
            vmem=2,
            name="finish",
        )(*sums)
        return (output, latent_grad, down, up, down_proj, up_proj)

    return layer


def solution(mesh):
    block = P("runs", "lat", "lon", None)
    sizes = (mesh.shape["lon"], mesh.shape["lat"])
    return jax.shard_map(
        on_device(sizes),
        mesh=mesh,
        in_specs=(block, block, P("runs", "lat", "lon")) + (P(),) * 8,
        out_specs=(block, block) + (P("runs", None),) * 4,
        check_vma=False,
    )
```

```python
import functools
import math

import jax
import jax.numpy as jnp
import numpy as np
from jax import lax
from jax.experimental import pallas as pl
from jax.experimental.pallas import tpu as pltpu
from jax.sharding import PartitionSpec as P

HEADS = 8
WIN_LEV = 2
WIN_LAT = 6
WIN_LON = 12
HALF_LAT = WIN_LAT // 2
HALF_LON = WIN_LON // 2
HALF_LEV = WIN_LEV // 2
WINDOW = WIN_LEV * WIN_LAT * WIN_LON


epsilon = 1e-05
masked_value = -1e30
f32 = jnp.float32
bf16 = jnp.bfloat16


def nn(a, b):
    return lax.dot_general(a, b, (((1,), (0,)), ((), ())), preferred_element_type=f32)


def nt(a, b):
    return lax.dot_general(a, b, (((1,), (1,)), ((), ())), preferred_element_type=f32)


def tn(a, b):
    return lax.dot_general(a, b, (((0,), (0,)), ((), ())), preferred_element_type=f32)


def call(kernel, out_shape, scratch=(), vmem=16, **kw):
    return pl.pallas_call(
        kernel,
        out_shape=out_shape,
        scratch_shapes=list(scratch),
        compiler_params=pltpu.CompilerParams(vmem_limit_bytes=vmem * 1024 * 1024),
        **kw,
    )


def in_hbm(array):
    return pltpu.with_memory_space_constraint(array, pltpu.HBM)


def struct(shape, dtype):
    return jax.ShapeDtypeStruct(shape, dtype)


ANY = pl.BlockSpec(memory_space=pl.ANY)
HBM = pl.BlockSpec(memory_space=pltpu.HBM)
VMEM = pl.BlockSpec(memory_space=pltpu.VMEM)


def corner(ref, quad):
    lat = 0 if quad >= 2 else HALF_LAT
    lon = 0 if quad % 2 else HALF_LON
    return ref.at[lat : lat + HALF_LAT, lon : lon + HALF_LON]


def run_copies(pairs, sems):
    copies = [pltpu.make_async_copy(src, dst, sems.at[i]) for i, (src, dst) in enumerate(pairs)]
    for copy in copies:
        copy.start()
    return copies


def pack_kernel(x_ref, g_ref, *refs):
    outs, sems = refs[:8], refs[8]
    pairs = [(corner(x_ref, q), outs[q]) for q in range(4)]
    pairs += [(corner(g_ref, q), outs[4 + q]) for q in range(4)]
    for copy in run_copies(pairs, sems):
        copy.wait()


def pack(x, g):
    _, _, levels, width = x.shape
    quads = call(
        pack_kernel,
        [struct((HALF_LAT, HALF_LON, levels, width), bf16)] * 8,
        [pltpu.SemaphoreType.DMA((8,))],
        vmem=2,
        in_specs=[HBM] * 2,
        out_specs=[ANY] * 8,
        name="pack",
    )(in_hbm(x), in_hbm(g))
    return quads[:4], quads[4:]


JOINED = (1, 2, 3)
APART = tuple(quad for quad in range(1, 4) if quad not in JOINED)


def unpack_kernel(*refs):
    outs, sems = refs[-3:-1], refs[-1]
    pairs = []
    for i, quad in enumerate((0,) + APART):
        for n in range(2):
            pairs.append((refs[2 * i + n], corner(outs[n], quad)))
    for i, quad in enumerate(JOINED):
        for n in range(2):
            pairs.append((refs[2 + 2 * len(APART) + i].at[n], corner(outs[n], quad)))
    for copy in run_copies(pairs, sems):
        copy.wait()


def unpack(out, back, shape):
    arrays = []
    for quad in (0,) + APART:
        arrays += [out[quad], back[quad]]
    arrays += [back[quad] for quad in JOINED]
    return call(
        unpack_kernel,
        [struct(shape, bf16)] * 2,
        [pltpu.SemaphoreType.DMA((8,))],
        vmem=2,
        in_specs=[ANY] * len(arrays),
        out_specs=[ANY] * 2,
        name="unpack",
    )(*arrays)


AXES = (WIN_LEV, WIN_LAT, WIN_LON)
PLACES = sum(AXES)
SPLITS = 3
MARK = SPLITS * PLACES
LANES = 128


def score_constants():
    n = np.arange(WINDOW)
    lev, r = n // (WINDOW // WIN_LEV), n % (WINDOW // WIN_LEV)
    quad, s = r // (HALF_LAT * HALF_LON), r % (HALF_LAT * HALF_LON)
    lat = (quad // 2) * HALF_LAT + s // HALF_LON
    lon = (quad % 2) * HALF_LON + s % HALF_LON
    starts = (0, WIN_LEV, WIN_LEV + WIN_LAT)
    place = np.zeros((WINDOW, PLACES), np.float32)
    for start, where in zip(starts, (lev, lat, lon)):
        place[n, start + where] = 1
    axis_of = np.repeat(np.arange(3), AXES)
    spot = np.concatenate([np.arange(extent) for extent in AXES])
    bases = (WIN_LEV - 1, 2 * WIN_LEV - 1 + WIN_LAT - 1, 2 * WIN_LEV + 2 * WIN_LAT - 2 + WIN_LON - 1)
    column = np.full((PLACES, HEADS, LANES), -1, np.int32)
    for key in range(PLACES):
        for query in range(PLACES):
            if axis_of[key] == axis_of[query]:
                at = bases[axis_of[key]] + spot[query] - spot[key]
                for part in range(SPLITS):
                    column[key, :, part * PLACES + query] = at
    spread = np.zeros((SPLITS, HEADS, HEADS, LANES), np.float32)
    for part in range(SPLITS):
        for h in range(HEADS):
            spread[part, h, h, part * PLACES : (part + 1) * PLACES] = 1
    query_side = np.zeros((WINDOW, LANES), np.float32)
    query_side[:, :MARK] = np.tile(place, (1, SPLITS))
    first = lev == 0
    lat_of = place[first][:, WIN_LEV : WIN_LEV + WIN_LAT]
    lon_of = place[first][:, WIN_LEV + WIN_LAT :]
    return (
        jnp.asarray(column.reshape(PLACES, HEADS * LANES)),
        jnp.asarray(spread.reshape(SPLITS, HEADS, HEADS * LANES), bf16),
        jnp.asarray(place, bf16),
        jnp.asarray(query_side, f32),
        jnp.asarray(lat_of, f32),
        jnp.asarray(lon_of, f32),
    )


def table_kernel(*refs, count):
    inputs, refs = refs[: 8 + count], refs[8 + count :]
    key_out, query_out = refs[:2]
    kept, local, sems = refs[2 : 2 + count], refs[2 + count : 10 + count], refs[10 + count]
    copies = run_copies(list(zip(inputs, tuple(local) + tuple(kept))), sems)
    for copy in copies[:8]:
        copy.wait()
    make_columns(*local, key_out, query_out)
    for copy in copies[8:]:
        copy.wait()


def make_columns(
    pb_ref, ids_ref, column_ref, spread_ref, place_ref, query_ref, lat_ref, lon_ref, key_out, query_out
):
    windows = key_out.shape[0]
    rest = pb_ref[...]
    wide = None
    for part in range(SPLITS):
        piece = rest.astype(bf16)
        rest = rest - piece.astype(f32)
        term = tn(piece, spread_ref[part])
        wide = term if wide is None else wide + term
    column = column_ref[...]
    table = jnp.zeros(column.shape, f32)
    for c in range(pb_ref.shape[1]):
        table = jnp.where(column == c, wide[c : c + 1, :], table)
    keys = nn(place_ref[...], table.astype(bf16))
    ids = None
    for lat in range(WIN_LAT):
        term = lat_ref[:, lat : lat + 1] * nt(lon_ref[...], ids_ref[lat].astype(f32))
        ids = term if ids is None else ids + term
    half = WINDOW // WIN_LEV
    lane = lax.broadcasted_iota(jnp.int32, (half, LANES), 1)
    for w in range(windows):
        key_rows, query_rows = [], []
        for lev in range(WIN_LEV):
            mine = ids[:, w * WIN_LEV + lev : w * WIN_LEV + lev + 1]
            rows = slice(lev * half, (lev + 1) * half)
            mask = jnp.where(
                lane == MARK,
                masked_value * mine,
                jnp.where(lane == MARK + 1, masked_value * (1.0 - mine), 0.0),
            )
            key_rows.append(
                jnp.concatenate(
                    [keys[rows, h * LANES : (h + 1) * LANES] + mask for h in range(HEADS)], 1
                )
            )
            query_rows.append(
                jnp.where(
                    lane == MARK,
                    1.0 - mine,
                    jnp.where(lane == MARK + 1, mine, query_ref[rows, :]),
                )
            )
        key_out[w] = jnp.concatenate(key_rows, 0).astype(bf16)
        query_out[w] = jnp.concatenate(query_rows, 0).astype(bf16)


def score_columns(position_bias, mask_ids, weights):
    windows = mask_ids.shape[0] // WIN_LEV
    inputs = (position_bias, mask_ids.transpose(1, 0, 2)) + score_constants()
    return call(
        functools.partial(table_kernel, count=len(weights)),
        [struct((windows, WINDOW, HEADS * LANES), bf16), struct((windows, WINDOW, LANES), bf16)]
        + [struct(w.shape, w.dtype) for w in weights],
        [pltpu.VMEM(x.shape, x.dtype) for x in inputs]
        + [pltpu.SemaphoreType.DMA((len(inputs) + len(weights),))],
        in_specs=[HBM] * (len(inputs) + len(weights)),
        name="table",
    )(*map(in_hbm, inputs), *map(in_hbm, weights))


def slabs(quads):
    _, _, levels, _ = quads[0].shape
    for quad in range(4):
        for lat in range(HALF_LAT):
            for lon in range(HALF_LON):
                yield quads[quad], lat, lon, ((quad * HALF_LAT + lat) * HALF_LON + lon) * levels


def gather_rows(quads, scratch, out_ref):
    levels = quads[0].shape[2]
    tiles, total, _ = scratch.shape
    rows = total // levels
    for ref, lat, lon, at in slabs(quads):
        slab = ref[lat, lon].astype(f32)
        for t in range(tiles):
            scratch[t, at : at + levels, :] = slab[:, t * LANES : (t + 1) * LANES]
    for level in range(levels):
        for t in range(tiles):
            out_ref[level * rows : (level + 1) * rows, t * LANES : (t + 1) * LANES] = scratch[
                t, pl.ds((level + HALF_LEV) % levels, rows, stride=levels), :
            ]


def scatter_rows(value, scratch, outs):
    levels = outs[0].shape[2]
    tiles, total, _ = scratch.shape
    rows = total // levels
    for level in range(levels):
        for t in range(tiles):
            scratch[t, pl.ds((level + HALF_LEV) % levels, rows, stride=levels), :] = value[
                level * rows : (level + 1) * rows, t * LANES : (t + 1) * LANES
            ]
    for ref, lat, lon, at in slabs(outs):
        for t in range(tiles):
            ref[lat, lon, :, t * LANES : (t + 1) * LANES] = scratch[t, at : at + levels, :].astype(bf16)


def forward_kernel(
    x0, x1, x2, x3, key_cols, query_cols, gain, w_qkv, qkv_down, qkv_up, w_proj, proj_down, proj_up,
    o0, o1, o2, o3, unit_ref, inv_ref, normed_ref, low_ref, qkv_ref, probs_ref, attn_ref, low_proj_ref,
    scratch, rows_ref, scores_ref, rounded_ref,
):
    gather_rows((x0, x1, x2, x3), scratch, rows_ref)
    total, width = rows_ref.shape
    windows = total // WINDOW
    head = width // HEADS
    pair = 2 * head
    for w in range(windows):
        at = slice(w * WINDOW, (w + 1) * WINDOW)
        rows = rows_ref[at, :]
        average = jnp.mean(rows, axis=-1, keepdims=True)
        centered = rows - average
        variance = jnp.mean(centered * centered, axis=-1, keepdims=True)
        inv_std = lax.rsqrt(variance + epsilon)
        unit = centered * inv_std
        normed = (unit * gain[...]).astype(bf16)
        unit_ref[at, :] = unit
        inv_ref[at, :] = inv_std
        normed_ref[at, :] = normed
        low = nt(normed, qkv_down[...]).astype(bf16)
        low_ref[at, :] = low
        qkv_ref[at, :] = (nn(normed, w_qkv[...]) + nn(low, qkv_up[...])).astype(bf16)
    scale = 1.0 / math.sqrt(head)
    assert math.frexp(scale)[0] == 0.5
    lane = lax.broadcasted_iota(jnp.int32, (WINDOW, pair), 1)
    pairs = [(w, p) for w in range(windows) for p in range(HEADS // 2)]

    def start(w, p):
        at = slice(w * WINDOW, (w + 1) * WINDOW)
        query = qkv_ref[at, p * pair : (p + 1) * pair] * jnp.asarray(scale, bf16)
        keys = qkv_ref[at, width + p * pair : width + (p + 1) * pair]
        for h in range(2):
            mine = (lane < head) if h == 0 else (lane >= head)
            number = 2 * p + h
            wide_query = jnp.concatenate([jnp.where(mine, query, 0), query_cols[w]], 1)
            wide_keys = jnp.concatenate(
                [keys, key_cols[w, :, number * LANES : (number + 1) * LANES]], 1
            )
            scores_ref[w * HEADS + number] = nt(wide_keys, wide_query)

    def middle(w, p):
        for h in range(2):
            index = w * HEADS + 2 * p + h
            scores = scores_ref[index]
            terms = jnp.exp(scores - jnp.max(scores, axis=0, keepdims=True))
            probs = terms * (1.0 / jnp.sum(terms, axis=0, keepdims=True))
            probs_ref[index] = probs
            rounded_ref[index] = probs.astype(bf16)

    def end(w, p):
        at = slice(w * WINDOW, (w + 1) * WINDOW)
        values = qkv_ref[at, 2 * width + p * pair : 2 * width + (p + 1) * pair]
        mixed = [tn(rounded_ref[w * HEADS + 2 * p + h], values) for h in range(2)]
        attn_ref[at, p * pair : (p + 1) * pair] = jnp.where(
            lane < head, mixed[0], mixed[1]
        ).astype(bf16)

    for stage in (start, middle, end):
        for w, p in pairs:
            stage(w, p)
    attn = attn_ref[...]
    low_proj = nt(attn, proj_down[...]).astype(bf16)
    low_proj_ref[...] = low_proj
    out = rows_ref[...] + nn(attn, w_proj[...]) + nn(low_proj, proj_up[...])
    scatter_rows(out, scratch, (o0, o1, o2, o3))


def backward_kernel(
    g0, g1, g2, g3, normed_ref, low_ref, qkv_ref, probs_ref, attn_ref, low_proj_ref,
    qkv_up, w_proj, proj_down, proj_up,
    grad_ref, d_qkv_ref, d_low_ref, keep_ref, send_ref, scratch, probs_grad, scores_grad,
):
    gather_rows((g0, g1, g2, g3), scratch, grad_ref)
    width = grad_ref.shape[1]
    windows = grad_ref.shape[0] // WINDOW
    head = width // HEADS
    pair = 2 * head
    scale = 1.0 / math.sqrt(head)
    grad = grad_ref[...].astype(bf16)
    d_low_proj = nt(grad, proj_up[...]).astype(bf16)
    d_attn = (nt(grad, w_proj[...]) + nn(d_low_proj, proj_down[...])).astype(bf16)
    lane = lax.broadcasted_iota(jnp.int32, (WINDOW, pair), 1)
    pairs = [(w, p) for w in range(windows) for p in range(HEADS // 2)]

    def start(w, p):
        at = slice(w * WINDOW, (w + 1) * WINDOW)
        values = qkv_ref[at, 2 * width + p * pair : 2 * width + (p + 1) * pair]
        scaled = d_attn[at, p * pair : (p + 1) * pair] * jnp.asarray(scale, bf16)
        for h in range(2):
            mine = (lane < head) if h == 0 else (lane >= head)
            probs_grad[w * HEADS + 2 * p + h] = nt(values, jnp.where(mine, scaled, 0))

    def middle(w, p):
        for h in range(2):
            index = w * HEADS + 2 * p + h
            probs = probs_ref[index]
            d_probs = probs_grad[index]
            inner = jnp.sum(d_probs * probs, axis=0, keepdims=True)
            scores_grad[index] = (probs * (d_probs - inner)).astype(bf16)

    def end(w, p):
        at = slice(w * WINDOW, (w + 1) * WINDOW)
        cols = [slice(s * width + p * pair, s * width + (p + 1) * pair) for s in range(3)]
        query = qkv_ref[at, cols[0]]
        keys_t = qkv_ref[at, cols[1]].T
        d_out = d_attn[at, p * pair : (p + 1) * pair]
        d_q, d_k, d_v = [], [], []
        for h in range(2):
            index = w * HEADS + 2 * p + h
            d_scores = scores_grad[index]
            d_v.append(nn(probs_ref[index].astype(bf16), d_out))
            d_k.append(nn(d_scores, query))
            d_q.append(nn(keys_t[h * head : (h + 1) * head], d_scores).astype(bf16))
        d_qkv_ref[at, cols[0]] = jnp.concatenate(d_q, 0).T
        for s, parts in ((1, d_k), (2, d_v)):
            d_qkv_ref[at, cols[s]] = jnp.where(lane < head, parts[0], parts[1]).astype(bf16)

    for i in range(len(pairs) + 2):
        if i < len(pairs):
            start(*pairs[i])
        if 1 <= i <= len(pairs):
            middle(*pairs[i - 1])
        if i >= 2:
            end(*pairs[i - 2])
    d_qkv = d_qkv_ref[...]
    d_low = nt(d_qkv, qkv_up[...]).astype(bf16)
    d_low_ref[...] = d_low
    raw = jnp.concatenate(
        [
            tn(d_low, normed_ref[...]),
            tn(low_ref[...], d_qkv),
            tn(d_low_proj, attn_ref[...]),
            tn(low_proj_ref[...], grad),
        ],
        1,
    )
    half = keep_ref.shape[1]
    odd = lax.axis_index("lon") % 2

    @pl.when(odd == 0)
    def _():
        keep_ref[...] = raw[:, :half]
        send_ref[...] = raw[:, half:]

    @pl.when(odd == 1)
    def _():
        keep_ref[...] = raw[:, half:]
        send_ref[...] = raw[:, :half]


def norm_kernel(*refs):
    grad_ref, d_qkv_ref, d_low_ref, unit_ref, inv_ref, gain, w_qkv, qkv_down = refs[:8]
    outgoing, refs = refs[8 : 8 + len(JOINED)], refs[8 + len(JOINED) :]
    outs, scratch = list(refs[:4]), refs[4]
    copies = []
    if JOINED:
        pairs = [(src, outs[quad].at[0]) for src, quad in zip(outgoing, JOINED)]
        copies = run_copies(pairs, refs[5])
        for quad in JOINED:
            outs[quad] = outs[quad].at[1]
    d_normed = nt(d_qkv_ref[...], w_qkv[...]) + nn(d_low_ref[...], qkv_down[...])
    d_unit = d_normed * gain[...]
    unit = unit_ref[...]
    back = inv_ref[...] * (
        d_unit
        - jnp.mean(d_unit, axis=-1, keepdims=True)
        - unit * jnp.mean(d_unit * unit, axis=-1, keepdims=True)
    )
    scatter_rows(grad_ref[...] + back, scratch, outs)
    for copy in copies:
        copy.wait()


def step_pairs(mesh_shape, lon_by, lat_by):
    lons, lats = mesh_shape
    return [
        (i * lats + j, (i + lon_by) % lons * lats + (j + lat_by) % lats)
        for i in range(lons)
        for j in range(lats)
    ]


def exchange(quads, sizes, by):
    moved = dict(quads)
    for quad in moved:
        if quad:
            pairs = step_pairs(sizes, by * (quad % 2), by * (quad // 2))
            moved[quad] = lax.ppermute(moved[quad], ("lon", "lat"), pairs)
    return moved


def swap(value, axis, length, bit):
    return lax.ppermute(value, axis, [(i, i ^ bit) for i in range(length)])


def sum_over(keep, send, sizes):
    lons, lats = sizes
    total = keep + swap(send, "lon", lons, 1)
    steps = [("lat", lats, bit) for bit in powers(1, lats)]
    steps += [("lon", lons, bit) for bit in powers(2, lons)]
    for axis, length, bit in steps:
        raw = total.astype(bf16)
        other = swap(raw, axis, length, bit)
        total = raw.astype(f32) + other.astype(f32)
    return raw, other, swap(raw, axis, length, 1), swap(raw, axis, length, bit ^ 1)


def powers(bit, length):
    while bit < length:
        yield bit
        bit *= 2


def finish_kernel(raw_ref, other_ref, next_raw_ref, next_other_ref, *outs, scale):
    half = raw_ref.shape[1]
    odd = lax.axis_index("lon") % 2
    mine = raw_ref[...].astype(f32) + other_ref[...].astype(f32)
    theirs = next_raw_ref[...].astype(f32) + next_other_ref[...].astype(f32)

    def write(first, second):
        start = 0
        for out in outs:
            stop = start + out.shape[1]
            if start < half:
                cut = min(stop, half)
                out[:, : cut - start] = first[:, start:cut] * scale
            if stop > half:
                cut = max(start, half)
                out[:, cut - start :] = second[:, cut - half : stop - half] * scale
            start = stop

    @pl.when(odd == 0)
    def _():
        write(mine, theirs)

    @pl.when(odd == 1)
    def _():
        write(theirs, mine)


def on_device(sizes):
    def layer(
        latent, cotangent, mask_ids, position_bias, norm_gain,
        w_qkv, qkv_down, qkv_up, w_proj, proj_down, proj_up,
    ):
        levels, lat_rows, lon_cols, width = latent.shape
        assert (lat_rows, lon_cols) == (WIN_LAT, WIN_LON)
        windows = levels // WIN_LEV
        total = windows * WINDOW
        rank = qkv_down.shape[0]
        quarter = struct((HALF_LAT, HALF_LON, levels, width), bf16)
        columns = pltpu.VMEM((width // LANES, total, LANES), f32)
        x_quads, g_quads = pack(latent.transpose(1, 2, 0, 3), cotangent.transpose(1, 2, 0, 3))
        x_quads = exchange(enumerate(x_quads), sizes, -1).values()
        g_quads = exchange(enumerate(g_quads), sizes, -1).values()
        key_cols, query_cols, *weights = score_columns(
            position_bias,
            mask_ids,
            (norm_gain[None, :], w_qkv, qkv_down, qkv_up, w_proj, proj_down, proj_up),
        )
        gain, w_qkv, qkv_down, qkv_up, w_proj, proj_down, proj_up = weights
        (
            o0, o1, o2, o3, unit, inv_std, normed, low, qkv, probs, attn, low_proj,
        ) = call(
            forward_kernel,
            [quarter] * 4
            + [
                struct((total, width), f32),
                struct((total, 1), f32),
                struct((total, width), bf16),
                struct((total, rank), bf16),
                struct((total, 3 * width), bf16),
                struct((windows * HEADS, WINDOW, WINDOW), f32),
                struct((total, width), bf16),
                struct((total, rank), bf16),
            ],
            [
                columns,
                pltpu.VMEM((total, width), f32),
                pltpu.VMEM((windows * HEADS, WINDOW, WINDOW), f32),
                pltpu.VMEM((windows * HEADS, WINDOW, WINDOW), bf16),
            ],
            name="forward",
        )(*x_quads, key_cols, query_cols, *weights)
        out = exchange({0: o0, **{q: (o1, o2, o3)[q - 1] for q in APART}}, sizes, 1)
        grad, d_qkv, d_low, keep, send = call(
            backward_kernel,
            [
                struct((total, width), f32),
                struct((total, 3 * width), bf16),
                struct((total, rank), bf16),
                struct((rank, 3 * width), f32),
                struct((rank, 3 * width), f32),
            ],
            [
                columns,
                pltpu.VMEM((windows * HEADS, WINDOW, WINDOW), f32),
                pltpu.VMEM((windows * HEADS, WINDOW, WINDOW), bf16),
            ],
            name="backward",
        )(*g_quads, normed, low, qkv, probs, attn, low_proj, qkv_up, w_proj, proj_down, proj_up)
        sums = sum_over(keep, send, sizes)
        shapes = [quarter] * 4
        for quad in JOINED:
            shapes[quad] = struct((2,) + quarter.shape, bf16)
        back = call(
            norm_kernel,
            shapes,
            [columns] + [pltpu.SemaphoreType.DMA((len(JOINED),))] * bool(JOINED),
            in_specs=[pl.BlockSpec()] * 8 + [ANY] * len(JOINED),
            name="norm_back",
        )(grad, d_qkv, d_low, unit, inv_std, gain, w_qkv, qkv_down, *[(o1, o2, o3)[q - 1] for q in JOINED])
        back = exchange(enumerate(back), sizes, 1)
        output, latent_grad = unpack(out, back, (lat_rows, lon_cols, levels, width))
        output, latent_grad = (x.transpose(2, 0, 1, 3) for x in (output, latent_grad))
        grad_scale = 1.0 / math.sqrt(levels * lat_rows * lon_cols * sizes[0] * sizes[1])
        down, up, down_proj, up_proj = call(
            functools.partial(finish_kernel, scale=grad_scale),
            [struct((rank, n * width), f32) for n in (1, 3, 1, 1)],
            vmem=2,
            name="finish",
        )(*sums)
        return (output, latent_grad, down, up, down_proj, up_proj)

    return layer


def solution(mesh):
    block = P("runs", "lat", "lon", None)
    sizes = (mesh.shape["lon"], mesh.shape["lat"])
    return jax.shard_map(
        on_device(sizes),
        mesh=mesh,
        in_specs=(block, block, P("runs", "lat", "lon")) + (P(),) * 8,
        out_specs=(block, block) + (P("runs", None),) * 4,
        check_vma=False,
    )
```
